32 devices in a mesh: gx: 2 (over core), gy: 4 (over y, x), gz: 4 (over z).
Axes of the slice: x: 2, y: 2, z: 4, core: 2. Of those that a mesh axis runs over, the one named last changes fastest.
Arguments:
- block_values: bfloat16 [4, 64, 4, 6, 128, 128], P('gy', 'gx', 'gz'), as said below
- block_cols: int32 [4, 64, 4, 6], P('gy', 'gx', 'gz'), may hold values from 0 to 63, as said below
Outputs:
- purified: float32 [256, 32768], P(('gx', 'gy'), 'gz')
The draws below stay inside these ranges and needn't reach their ends.
Inputs may be any that keep to these rules, and one draw needn't show every extreme that they name: block_cols[a, s, b, :] holds 6 distinct tile columns of panel b at which tile row a * 64 + s of P is nonzero; every tile column of a panel is listed by exactly 6 tile rows of each slab; the pattern is symmetric: tile (i, j) is listed exactly when tile (j, i) is. `block_values`: P is symmetric: the tile listed at (i, j) is the transpose of the tile listed at (j, i), and diagonal tiles are symmetric.
All inputs are finite; a program needn't handle non-finite values.
Results may differ from the reference program's by a relative error of at most 0.0033.
Values may be sent and summed in bfloat16 or wider, within the bound.
A program may use at most 128 MiB of HBM per device.

```python
import jax
import jax.numpy as jnp
from jax import lax

TILE = 128
NT = 256
KP = 6
WIN = 1
NPAN = 4
ST = 64
RB = 32
ORDER = 32768
N_GX = 2


def tile_pattern(key):
    pattern_key = jax.random.fold_in(key, 11)
    split_keys = jax.random.split(pattern_key, 2)
    order_keys = jax.random.split(split_keys[0], NPAN * NPAN * 2)
    orders = jax.vmap(lambda subkey: jax.random.permutation(subkey, ST))(order_keys).reshape(NPAN, NPAN, 2, ST)
    first = orders[:, :, 0].astype(jnp.int32)
    second = orders[:, :, 1].astype(jnp.int32)
    slab_index = jnp.arange(NPAN, dtype=jnp.int32)[:, None, None]
    panel_index = jnp.arange(NPAN, dtype=jnp.int32)[None, :, None]
    lower_part = slab_index > panel_index
    on_diagonal = slab_index == panel_index
    first_swapped = jnp.swapaxes(first, 0, 1)
    second_swapped = jnp.swapaxes(second, 0, 1)
    source_order = jnp.where(lower_part, second_swapped, first)
    target_order = jnp.where(lower_part, first_swapped, jnp.where(on_diagonal, first, second))
    target_inverse = jnp.argsort(target_order, axis=-1).astype(jnp.int32)
    extra_shifts = (jax.random.permutation(split_keys[1], ST // 2 - 1)[:(KP - 2) // 2] + 1).astype(jnp.int32)
    shifts = jnp.concatenate([jnp.array([0, ST // 2], jnp.int32), extra_shifts, -extra_shifts])
    position = (source_order[:, :, :, None] + shifts[None, None, None, :]) % ST
    columns = jnp.take_along_axis(target_inverse, position.reshape(NPAN, NPAN, ST * KP), axis=2)
    return jnp.transpose(columns.reshape(NPAN, NPAN, ST, KP), (0, 2, 1, 3)).astype(jnp.int32)


def draw_block_cols(key, part):
    return tile_pattern(key)


def draw_block_values(key, part):
    columns = tile_pattern(key)
    row_global = jnp.broadcast_to((jnp.arange(NPAN, dtype=jnp.int32)[:, None] * ST + jnp.arange(ST, dtype=jnp.int32)[None, :])[:, :, None, None], (NPAN, ST, NPAN, KP))
    col_global = jnp.arange(NPAN, dtype=jnp.int32)[None, None, :, None] * ST + columns
    tile_ident = (jnp.minimum(row_global, col_global) * NT + jnp.maximum(row_global, col_global)).reshape(-1)
    value_key = jax.random.fold_in(key, 23)

    def one_tile(ident):
        subkey = jax.random.fold_in(value_key, ident)
        return jax.random.normal(subkey, (TILE, TILE), jnp.float32)
    raw_tiles = jax.vmap(one_tile)(tile_ident)
    flipped = (row_global > col_global).reshape(-1)[:, None, None]
    diagonal_mask = (row_global == col_global).reshape(-1)[:, None, None]
    swapped = jnp.swapaxes(raw_tiles, 1, 2)
    tiles = jnp.where(flipped, swapped, raw_tiles)
    tiles = jnp.where(diagonal_mask, (raw_tiles + swapped) * 0.7071, tiles)
    scale = 2.0 / (NPAN * KP * TILE) ** 0.5
    return (tiles * scale).reshape(NPAN, ST, NPAN, KP, TILE, TILE).astype(jnp.bfloat16)


def setup_inputs(seed: int = 0) -> dict:
    splits = jax.random.split(jax.random.key(seed), 3)
    return {
        "block_values": draw_block_values(jax.random.fold_in(splits[2], 71), 0),
        "block_cols": draw_block_cols(jax.random.fold_in(splits[2], 71), 0),
    }


def dense_rows(row_tiles, row_columns):
    count_rows = row_tiles.shape[0]
    global_cols = (jnp.arange(NPAN, dtype=jnp.int32)[None, :, None] * ST + row_columns).reshape(count_rows, NPAN * KP)
    onehot = (global_cols[:, :, None] == jnp.arange(NT, dtype=jnp.int32)[None, None, :]).astype(jnp.float32)
    flattened = row_tiles.reshape(count_rows, NPAN * KP, TILE, TILE).astype(jnp.float32)
    densified = jnp.einsum("nqj,nqyx->nyjx", onehot, flattened)
    return densified.reshape(count_rows * TILE, ORDER)


def times_matrix(left_rows, block_values, block_cols):
    height = left_rows.shape[0]
    all_tiles = block_values.reshape(NT, NPAN * KP, TILE, TILE)
    all_columns = (jnp.arange(NPAN, dtype=jnp.int32)[None, :, None] * ST + block_cols.reshape(NT, NPAN, KP)).reshape(NT, NPAN * KP)

    def advance(running, inputs):
        row_tiles, row_columns, tile_row = inputs
        portion = lax.dynamic_slice_in_dim(left_rows, tile_row * TILE, TILE, 1)
        product = jnp.einsum("rx,qxy->rqy", portion, row_tiles.astype(jnp.float32))
        return running.at[:, row_columns, :].add(product), None

    running = jnp.zeros((height, NT, TILE), jnp.float32)
    running, ignored = lax.scan(advance, running, (all_tiles, all_columns, jnp.arange(NT, dtype=jnp.int32)))
    return running.reshape(height, ORDER)


def reference(block_values, block_cols):
    window_index = (jnp.arange(N_GX, dtype=jnp.int32)[:, None] * RB + jnp.arange(WIN, dtype=jnp.int32)[None, :]).reshape(-1)
    left_rows = dense_rows(block_values[0][window_index], block_cols[0][window_index])
    square = times_matrix(left_rows, block_values, block_cols)
    rounded = lax.optimization_barrier(square.astype(jnp.bfloat16)).astype(jnp.float32)
    return 3.0 * square - 2.0 * times_matrix(rounded, block_values, block_cols)
```

```python
import functools

import jax
import jax.numpy as jnp
from jax import lax
from jax.experimental import pallas as pl
from jax.experimental.pallas import tpu as pltpu
from jax.sharding import PartitionSpec as P

LANES = 128
SUB = 8
MESH = pl.DeviceIdType.MESH
HOP_LAG, SIDE_LAG, LAST_LAG = 3, 2, 3
PIECES = 8


def pieces_of(count, most):
    for pieces in range(min(count, most), 0, -1):
        if count % pieces == 0:
            return pieces


def greet(axes):
    barrier = pltpu.get_barrier_semaphore()
    total = 0
    for axis in axes:
        size = lax.axis_size(axis)
        me = lax.axis_index(axis)
        for step in range(1, size):
            pl.semaphore_signal(
                barrier, inc=1, device_id={axis: lax.rem(me + step, size)}, device_id_type=MESH
            )
        total += size - 1
    pl.semaphore_wait(barrier, total)


def remote(src, dst, send, recv, axis, peer):
    return pltpu.make_async_remote_copy(
        src_ref=src, dst_ref=dst, send_sem=send, recv_sem=recv,
        device_id={axis: peer}, device_id_type=MESH,
    )


def step_kernel(
    n_gx, n_gy, n_gz, slots, pieces, buffers,
    tiles, cols, out,
    held, window, current, heads, table_v, lists_v, table, lists,
    own, right_out, left_out, right_in, left_in, square, rounded,
    product, side_out, side_in, mixed, last_out, last_in,
    load_sem, head_sem, head_side, win_send, win_recv, fan_send, fan_recv, table_sem,
    right_send, left_send, right_recv, left_recv, side_send, side_recv, last_send, last_recv, credit,
):
    gx, gy, gz = lax.axis_index("gx"), lax.axis_index("gy"), lax.axis_index("gz")
    rows = tiles.shape[0]
    size = tiles.shape[2]
    count = n_gx * rows
    chunks = window.shape[0]
    high = n_gy * SUB
    wide = rows // pieces
    broad = count // pieces
    steps = chunks * pieces
    f32, bf16 = jnp.float32, jnp.bfloat16

    first_load = pltpu.make_async_copy(tiles.at[0], held.at[pl.ds(0, slots)], load_sem.at[0])
    first_load.start()
    loads = [first_load]
    for r in range(1, rows):
        loads.append(pltpu.make_async_copy(tiles.at[r], held.at[pl.ds(r * slots, slots)], load_sem.at[r]))
        loads[-1].start()
    greet(("gx", "gy", "gz"))

    def win_copy(m, peer):
        return remote(window.at[m, gx], window.at[m, gx], win_send.at[m, peer], win_recv.at[m], "gy", peer)

    def fan_copy(m, d):
        return remote(window.at[m, gx], window.at[m, gx], fan_send.at[m, d - 1], fan_recv.at[m, d - 1],
                      "gx", lax.rem(gx + d, n_gx))

    def fan_landing(m, d):
        g = lax.rem(gx - d + n_gx, n_gx)
        return remote(window.at[m, g], window.at[m, g], fan_send.at[m, d - 1], fan_recv.at[m, d - 1],
                      "gx", lax.rem(gx + d, n_gx))

    def head_copy(peer):
        return remote(heads.at[gx], heads.at[gx], head_sem.at[0, peer], head_sem.at[1, 0], "gy", peer)

    def head_fan(d):
        return remote(heads.at[gx], heads.at[gx], head_side.at[0, d - 1], head_side.at[1, d - 1],
                      "gx", lax.rem(gx + d, n_gx))

    def head_landing(d):
        g = lax.rem(gx - d + n_gx, n_gx)
        return remote(heads.at[g], heads.at[g], head_side.at[0, d - 1], head_side.at[1, d - 1],
                      "gx", lax.rem(gx + d, n_gx))

    @pl.when(gy == 0)
    def _():
        heads[gx] = cols[pl.ds(0, heads.shape[1])]
        for peer in range(1, n_gy):
            head_copy(peer).start()
        for d in range(1, n_gx):
            head_fan(d).start()
        first_load.wait()
        for k in range(slots):
            tile = held[k].astype(f32)
            for m in range(chunks):
                window[m, gx, k] = jnp.concatenate(
                    [tile[q * chunks * SUB + m * SUB:][:SUB] for q in range(n_gy)], axis=0
                ).astype(bf16)
        for m in range(chunks):
            for peer in range(1, n_gy):
                win_copy(m, peer).start()
            for d in range(1, n_gx):
                fan_copy(m, d).start()

    lanes = lax.broadcasted_iota(jnp.int32, (rows, LANES), 1)
    places = lax.broadcasted_iota(jnp.int32, (rows, LANES), 0)
    listed = cols[...]
    marks = [
        jnp.where(jnp.broadcast_to(listed[:, k:k + 1], (rows, LANES)) == lanes, places * SUB + k, -1)
        for k in range(slots)
    ]
    lists_v[...] = jnp.zeros_like(lists_v)
    for i in range(slots):
        top = marks[0]
        for k in range(1, slots):
            top = jnp.maximum(top, marks[k])
        top = jnp.max(top, axis=0, keepdims=True)
        marks = [jnp.where(mark == top, -1, mark) for mark in marks]
        row, slot = top // SUB, top % SUB
        lists_v[i:i + 1] = jnp.where(top < 0, rows, row)
        lists_v[SUB + i:SUB + i + 1] = jnp.where(top < 0, 0, row * slots + slot)
    list_copy = pltpu.make_async_copy(lists_v, lists, table_sem.at[0])
    list_copy.start()
    for g in range(n_gx):
        current[g, slots] = jnp.zeros((high, size), bf16)
    for parity in range(2):
        rounded[parity, rows] = jnp.zeros((n_gx * high, size), bf16)

    @pl.when(gy != 0)
    def _():
        head_copy(0).wait_recv()
        for d in range(1, n_gx):
            head_fan(d).start()

    for d in range(1, n_gx):
        head_landing(d).wait_recv()
    total = jnp.zeros((rows, LANES), jnp.int32)
    for g in range(n_gx):
        found = jnp.full((rows, LANES), slots, jnp.int32)
        for k in range(slots):
            found = jnp.where(listed == jnp.broadcast_to(heads[g, 0:1, k:k + 1], (rows, LANES)), k, found)
        found = jnp.where(lanes < slots, found, 0)
        total = total + (found if g == 0 else pltpu.roll(found, g * SUB, 1))
    table_v[...] = total
    table_copy = pltpu.make_async_copy(table_v, table, table_sem.at[1])
    table_copy.start()

    def forward(m):
        @pl.when(gy != 0)
        def _():
            win_copy(m, 0).wait_recv()
            for d in range(1, n_gx):
                fan_copy(m, d).start()

    forward(0)
    for load in loads[1:]:
        load.wait()

    @pl.when(gy != 0)
    def _():
        first_load.wait()

    list_copy.wait()
    table_copy.wait()

    def right_copy(t):
        return remote(right_out.at[t], right_in.at[t], right_send.at[t], right_recv.at[t],
                      "gz", lax.rem(gz + 1, n_gz))

    def left_copy(t):
        return remote(left_out.at[t], left_in.at[t], left_send.at[t], left_recv.at[t],
                      "gz", lax.rem(gz + n_gz - 1, n_gz))

    def side_slot(u):
        return u if buffers == chunks else lax.rem(u, buffers * pieces)

    def side_copy(u, d):
        peer = lax.rem(gx + d, n_gx)
        s = side_slot(u)
        return remote(side_out.at[s, peer], side_in.at[s, d - 1], side_send.at[s, d - 1], side_recv.at[s, d - 1],
                      "gx", peer)

    def last_copy(v, d):
        peer = lax.rem(gy + d, n_gy)
        return remote(last_out.at[v, peer], last_in.at[v, d - 1], last_send.at[v, d - 1], last_recv.at[v, d - 1],
                      "gy", peer)

    def during(t):
        return (t >= 0) & (t < steps)

    def stage_own(t):
        m, q = t // pieces, lax.rem(t, pieces)

        @pl.when((q == 1 % pieces) & (m + 1 < chunks))
        def _():
            forward(m + 1)

        @pl.when(q == 0)
        def _():
            for d in range(1, n_gx):
                fan_landing(m, d).wait_recv()
            for g in range(n_gx):
                for k in range(slots):
                    current[g, k] = window[m, g, k]

        for i in range(wide):
            c = q * wide + i
            lhs = jnp.concatenate([
                jnp.concatenate([current[g, table[c, g * SUB + j]] for g in range(n_gx)], axis=0)
                for j in range(slots)
            ], axis=1)
            rhs = jnp.concatenate([held[c * slots + j] for j in range(slots)], axis=1)
            own[t, i] = lax.dot_general(lhs, rhs, (((1,), (1,)), ((), ())), preferred_element_type=f32)

    def stage_right(t):
        @pl.when(gz == 0)
        def _():
            right_out[t] = own[t].astype(bf16)

        @pl.when(gz > 0)
        def _():
            right_copy(t).wait_recv()

        @pl.when((gz > 0) & (gz < n_gz - 1))
        def _():
            right_out[t] = (own[t] + right_in[t].astype(f32)).astype(bf16)

        @pl.when(gz < n_gz - 1)
        def _():
            right_copy(t).start()

    def stage_left(t):
        @pl.when(gz == n_gz - 1)
        def _():
            left_out[t] = own[t].astype(bf16)

        @pl.when(gz < n_gz - 1)
        def _():
            left_copy(t).wait_recv()

        @pl.when((gz > 0) & (gz < n_gz - 1))
        def _():
            left_out[t] = (own[t] + left_in[t].astype(f32)).astype(bf16)

        @pl.when(gz > 0)
        def _():
            left_copy(t).start()

    def stage_sum(t):
        parity, q = lax.rem(t // pieces, 2), lax.rem(t, pieces)

        def keep(total):
            square[parity, pl.ds(q * wide, wide)] = total
            rounded[parity, pl.ds(q * wide, wide)] = total.astype(bf16)

        @pl.when(gz == 0)
        def _():
            keep(own[t] + left_in[t].astype(f32))

        @pl.when(gz == n_gz - 1)
        def _():
            keep(own[t] + right_in[t].astype(f32))

        @pl.when((gz > 0) & (gz < n_gz - 1))
        def _():
            keep(own[t] + right_in[t].astype(f32) + left_in[t].astype(f32))

    def stage_second(u):
        parity, q = lax.rem(u // pieces, 2), lax.rem(u, pieces)
        depth = min(slots, rows)
        s = side_slot(u)
        hold = lax.rem(u, SIDE_LAG + 1)
        if buffers < chunks:
            @pl.when((q == 0) & (u >= buffers * pieces))
            def _():
                pl.semaphore_wait(credit, n_gx - 1)

            @pl.when(u >= buffers * pieces)
            def _():
                for d in range(1, n_gx):
                    side_copy(u, d).wait_send()

        for i in range(broad):
            c = q * broad + i
            lhs = jnp.concatenate([rounded[parity, lists[j, c]] for j in range(depth)], axis=1)
            rhs = jnp.concatenate([held[lists[SUB + j, c]] for j in range(depth)], axis=0)
            near = c - gx * rows
            here = (gy == gz) & (near >= 0) & (near < rows)
            near = jnp.clip(near, 0, rows - 1)
            value = (jnp.where(here, 3.0, 0.0) * square[parity, near]
                     - 2.0 * jnp.dot(lhs, rhs, preferred_element_type=f32))
            mine = value[:high]
            for g in range(1, n_gx):
                mine = jnp.where(gx == g, value[g * high:(g + 1) * high], mine)
            product[hold, i] = mine
            for g in range(n_gx):
                side_out[s, g, i] = value[g * high:(g + 1) * high].astype(bf16)
        for d in range(1, n_gx):
            side_copy(u, d).start()

    def stage_mix(v):
        m, q = v // pieces, lax.rem(v, pieces)
        hold = lax.rem(v, SIDE_LAG + 1)
        s = side_slot(v)
        for d in range(1, n_gx):
            side_copy(v, d).wait_recv()
        for i in range(0, broad, 2):
            pair = []
            for h in range(i, i + 2):
                value = product[hold, h]
                for d in range(1, n_gx):
                    value = value + side_in[s, d - 1, h].astype(f32)
                mixed[h] = value
                pair.append(value)
            for y in range(n_gy):
                last_out[v, y, i // 2] = jnp.concatenate(
                    [value[y * SUB:(y + 1) * SUB] for value in pair], axis=0
                ).astype(bf16)
        for d in range(1, n_gy):
            last_copy(v, d).start()
        if buffers < chunks:
            @pl.when((q == pieces - 1) & (m + buffers < chunks))
            def _():
                for d in range(1, n_gx):
                    pl.semaphore_signal(credit, inc=1, device_id={"gx": lax.rem(gx + d, n_gx)},
                                        device_id_type=MESH)
        down = pl.ds(pl.multiple_of(m * SUB, SUB), SUB)
        for i in range(broad):
            across = pl.ds(pl.multiple_of((q * broad + i) * size, size), size)
            out[down, across] = mixed[i, pl.ds(pl.multiple_of(gy * SUB, SUB), SUB)]

    def stage_last(w):
        m, q = w // pieces, lax.rem(w, pieces)
        for d in range(1, n_gy):
            last_copy(w, d).wait_recv()
        down = pl.ds(pl.multiple_of(m * SUB, SUB), SUB)
        for i in range(0, broad, 2):
            value = last_in[w, 0, i // 2].astype(f32)
            for d in range(2, n_gy):
                value = value + last_in[w, d - 1, i // 2].astype(f32)
            for h in range(2):
                across = pl.ds(pl.multiple_of((q * broad + i + h) * size, size), size)
                out[down, across] += value[h * SUB:(h + 1) * SUB]

    sum_at = (n_gz - 1) * HOP_LAG
    second_at = sum_at + pieces
    mix_at = second_at + SIDE_LAG
    last_at = mix_at + LAST_LAG

    def slot(s, carry):
        for stage, delay in (
            (stage_own, 0),
            (stage_right, gz * HOP_LAG),
            (stage_left, (n_gz - 1 - gz) * HOP_LAG),
            (stage_sum, sum_at),
            (stage_mix, mix_at),
            (stage_second, second_at),
            (stage_last, last_at),
        ):
            pl.when(during(s - delay))(functools.partial(stage, s - delay))
        return carry

    lax.fori_loop(0, steps + last_at, slot, jnp.int32(0))

    @pl.loop(0, steps)
    def _(t):
        @pl.when(gz < n_gz - 1)
        def _():
            right_copy(t).wait_send()

        @pl.when(gz > 0)
        def _():
            left_copy(t).wait_send()

        for d in range(1, n_gy):
            last_copy(t, d).wait_send()

    @pl.loop(0, buffers * pieces)
    def _(t):
        for d in range(1, n_gx):
            side_copy(t, d).wait_send()

    for d in range(1, n_gx):
        head_fan(d).wait_send()
        for m in range(chunks):
            fan_copy(m, d).wait_send()

    @pl.when(gy == 0)
    def _():
        for peer in range(1, n_gy):
            head_copy(peer).wait_send()
            for m in range(chunks):
                win_copy(m, peer).wait_send()


def local(block_values, block_cols):
    n_gx, n_gy, n_gz = (lax.axis_size(a) for a in ("gx", "gy", "gz"))
    tiles = block_values[0, :, 0]
    cols = block_cols[0, :, 0]
    rows, slots, size = tiles.shape[:3]
    cols = jnp.pad(cols, ((0, 0), (0, LANES - slots)), constant_values=-1)
    count = n_gx * rows
    chunks = size // (n_gy * SUB)
    high = n_gy * SUB
    pieces = pieces_of(rows, PIECES)
    wide, broad, steps = rows // pieces, count // pieces, chunks * pieces
    tall = n_gx * high
    buffers = chunks if n_gx <= 4 else 2
    top = min(SUB, rows)
    dma = pltpu.SemaphoreType.DMA
    f32, bf16 = jnp.float32, jnp.bfloat16
    flow = (steps, wide, tall, size)
    return pl.pallas_call(
        functools.partial(step_kernel, n_gx, n_gy, n_gz, slots, pieces, buffers),
        out_shape=jax.ShapeDtypeStruct((size // n_gy, count * size), f32),
        in_specs=[pl.BlockSpec(memory_space=pl.ANY), pl.BlockSpec(memory_space=pltpu.VMEM)],
        out_specs=pl.BlockSpec(memory_space=pltpu.VMEM),
        scratch_shapes=[
            pltpu.VMEM((rows * slots, size, size), bf16),
            pltpu.VMEM((chunks, n_gx, slots, high, size), bf16),
            pltpu.VMEM((n_gx, slots + 1, high, size), bf16),
            pltpu.VMEM((n_gx, top, LANES), jnp.int32),
            pltpu.VMEM((rows, LANES), jnp.int32),
            pltpu.VMEM((2 * SUB, LANES), jnp.int32),
            pltpu.SMEM((rows, LANES), jnp.int32),
            pltpu.SMEM((2 * SUB, LANES), jnp.int32),
            pltpu.VMEM(flow, f32),
            pltpu.VMEM(flow, bf16), pltpu.VMEM(flow, bf16), pltpu.VMEM(flow, bf16), pltpu.VMEM(flow, bf16),
            pltpu.VMEM((2, rows, tall, size), f32),
            pltpu.VMEM((2, rows + 1, tall, size), bf16),
            pltpu.VMEM((SIDE_LAG + 1, broad, high, size), f32),
            pltpu.VMEM((buffers * pieces, n_gx, broad, high, size), bf16),
            pltpu.VMEM((buffers * pieces, n_gx - 1, broad, high, size), bf16),
            pltpu.VMEM((broad, high, size), f32),
            pltpu.VMEM((steps, n_gy, broad // 2, 2 * SUB, size), bf16),
            pltpu.VMEM((steps, n_gy - 1, broad // 2, 2 * SUB, size), bf16),
            dma((rows,)), dma((2, n_gy)), dma((2, n_gx - 1)),
            dma((chunks, n_gy)), dma((chunks,)), dma((chunks, n_gx - 1)), dma((chunks, n_gx - 1)), dma((2,)),
            dma((steps,)), dma((steps,)), dma((steps,)), dma((steps,)),
            dma((buffers * pieces, n_gx - 1)), dma((buffers * pieces, n_gx - 1)),
            dma((steps, n_gy - 1)), dma((steps, n_gy - 1)),
            pltpu.SemaphoreType.REGULAR,
        ],
        compiler_params=pltpu.CompilerParams(
            collective_id=0, has_side_effects=True, vmem_limit_bytes=67043328
        ),
        name="purify",
    )(tiles, cols)


def solution(mesh):
    in_specs = (P("gy", "gx", "gz", None, None, None), P("gy", "gx", "gz", None))
    out_specs = P(("gx", "gy"), "gz")
    return jax.shard_map(local, mesh=mesh, in_specs=in_specs, out_specs=out_specs, check_vma=False)
```

```python
import functools

import jax
import jax.numpy as jnp
from jax import lax
from jax.experimental import pallas as pl
from jax.experimental.pallas import tpu as pltpu
from jax.sharding import PartitionSpec as P

LANES = 128
SUB = 8
VMEM = 67043328
MESH = pl.DeviceIdType.MESH
HOP_LAG, SIDE_LAG, LAST_LAG = 3, 2, 6
PIECES = 8


def pieces_of(count, most):
    for pieces in range(min(count, most), 0, -1):
        if count % pieces == 0:
            return pieces


def greet(axes):
    barrier = pltpu.get_barrier_semaphore()
    total = 0
    for axis in axes:
        size = lax.axis_size(axis)
        me = lax.axis_index(axis)
        for step in range(1, size):
            pl.semaphore_signal(
                barrier, inc=1, device_id={axis: lax.rem(me + step, size)}, device_id_type=MESH
            )
        total += size - 1
    pl.semaphore_wait(barrier, total)


def remote(src, dst, send, recv, axis, peer):
    return pltpu.make_async_remote_copy(
        src_ref=src, dst_ref=dst, send_sem=send, recv_sem=recv,
        device_id={axis: peer}, device_id_type=MESH,
    )


def step_kernel(
    n_gx, n_gy, n_gz, slots, pieces, buffers,
    tiles, cols, out,
    held, window, current, heads, table_v, lists_v, table, lists,
    own, right_out, left_out, right_in, left_in, square, rounded,
    product, side_out, side_in, mixed, last_out, last_in,
    load_sem, head_sem, head_side, win_send, win_recv, fan_send, fan_recv, table_sem,
    right_send, left_send, right_recv, left_recv, side_send, side_recv, last_send, last_recv, credit,
):
    gx, gy, gz = lax.axis_index("gx"), lax.axis_index("gy"), lax.axis_index("gz")
    rows = cols.shape[3]
    size = tiles.shape[2]
    count = n_gx * rows
    chunks = window.shape[0]
    high = n_gy * SUB
    wide = rows // pieces
    broad = count // pieces
    steps = chunks * pieces
    f32, bf16 = jnp.float32, jnp.bfloat16

    first_load = pltpu.make_async_copy(tiles.at[pl.ds(0, slots)], held.at[pl.ds(0, slots)], load_sem.at[0])
    first_load.start()
    loads = [first_load]
    parts = load_sem.shape[0] - 1
    for part in range(parts):
        low, top = 1 + (rows - 1) * part // parts, 1 + (rows - 1) * (part + 1) // parts
        loads.append(pltpu.make_async_copy(
            tiles.at[pl.ds(low * slots, (top - low) * slots)], held.at[pl.ds(low * slots, (top - low) * slots)],
            load_sem.at[part + 1],
        ))
        loads[-1].start()
    greet(("gx", "gy", "gz"))

    def win_copy(m, peer):
        return remote(window.at[m, gx], window.at[m, gx], win_send.at[peer], win_recv.at[m], "gy", peer)

    def fan_copy(m, d):
        return remote(window.at[m, gx], window.at[m, gx], fan_send.at[d - 1], fan_recv.at[m, d - 1],
                      "gx", lax.rem(gx + d, n_gx))

    def fan_landing(m, d):
        g = lax.rem(gx - d + n_gx, n_gx)
        return remote(window.at[m, g], window.at[m, g], fan_send.at[d - 1], fan_recv.at[m, d - 1],
                      "gx", lax.rem(gx + d, n_gx))

    def head_copy(peer):
        return remote(heads.at[gx], heads.at[gx], head_sem.at[0, peer], head_sem.at[1, 0], "gy", peer)

    def head_fan(d):
        return remote(heads.at[gx], heads.at[gx], head_side.at[0, d - 1], head_side.at[1, d - 1],
                      "gx", lax.rem(gx + d, n_gx))

    def head_landing(d):
        g = lax.rem(gx - d + n_gx, n_gx)
        return remote(heads.at[g], heads.at[g], head_side.at[0, d - 1], head_side.at[1, d - 1],
                      "gx", lax.rem(gx + d, n_gx))

    lanes = lax.broadcasted_iota(jnp.int32, (rows, LANES), 1)
    places = lax.broadcasted_iota(jnp.int32, (rows, LANES), 0)
    listed = cols[0, :, 0, :].T
    each = [jnp.broadcast_to(listed[:, k:k + 1], (rows, LANES)) for k in range(slots)]
    spread = jnp.full((rows, LANES), -1, jnp.int32)
    for k in range(slots):
        spread = jnp.where(lanes == k, each[k], spread)

    @pl.when(gy == 0)
    def _():
        heads[gx] = spread[:heads.shape[1]]
        for peer in range(1, n_gy):
            head_copy(peer).start()
        for d in range(1, n_gx):
            head_fan(d).start()
        first_load.wait()
        for k in range(slots):
            tile = held[k].astype(f32)
            for m in range(chunks):
                window[m, gx, k] = jnp.concatenate(
                    [tile[q * chunks * SUB + m * SUB:][:SUB] for q in range(n_gy)], axis=0
                ).astype(bf16)
        for m in range(chunks):
            for peer in range(1, n_gy):
                win_copy(m, peer).start()
            for d in range(1, n_gx):
                fan_copy(m, d).start()

    marks = [jnp.where(each[k] == lanes, places * SUB + k, -1) for k in range(slots)]
    lists_v[...] = jnp.zeros_like(lists_v)
    for i in range(slots):
        top = marks[0]
        for k in range(1, slots):
            top = jnp.maximum(top, marks[k])
        top = jnp.max(top, axis=0, keepdims=True)
        marks = [jnp.where(mark == top, -1, mark) for mark in marks]
        row, slot = top // SUB, top % SUB
        lists_v[i:i + 1] = jnp.where(top < 0, rows, row)
        lists_v[SUB + i:SUB + i + 1] = jnp.where(top < 0, 0, row * slots + slot)
    list_copy = pltpu.make_async_copy(lists_v, lists, table_sem.at[0])
    list_copy.start()
    for g in range(n_gx):
        current[g, slots] = jnp.zeros((high, size), bf16)
    for parity in range(2):
        rounded[parity, rows] = jnp.zeros((n_gx * high, size), bf16)

    @pl.when(gy != 0)
    def _():
        head_copy(0).wait_recv()
        for d in range(1, n_gx):
            head_fan(d).start()

    for d in range(1, n_gx):
        head_landing(d).wait_recv()
    total = jnp.zeros((rows, LANES), jnp.int32)
    for g in range(n_gx):
        found = jnp.full((rows, LANES), slots, jnp.int32)
        for k in range(slots):
            found = jnp.where(spread == jnp.broadcast_to(heads[g, 0:1, k:k + 1], (rows, LANES)), k, found)
        found = jnp.where(lanes < slots, found, 0)
        total = total + (found if g == 0 else pltpu.roll(found, g * SUB, 1))
    table_v[...] = total
    table_copy = pltpu.make_async_copy(table_v, table, table_sem.at[1])
    table_copy.start()

    def forward(m):
        @pl.when(gy != 0)
        def _():
            win_copy(m, 0).wait_recv()
            for d in range(1, n_gx):
                fan_copy(m, d).start()

    forward(0)
    for load in loads[1:]:
        load.wait()

    @pl.when(gy != 0)
    def _():
        first_load.wait()

    list_copy.wait()
    table_copy.wait()

    def right_copy(t):
        return remote(right_out.at[t], right_in.at[t], right_send, right_recv.at[t],
                      "gz", lax.rem(gz + 1, n_gz))

    def left_copy(t):
        return remote(left_out.at[t], left_in.at[t], left_send, left_recv.at[t],
                      "gz", lax.rem(gz + n_gz - 1, n_gz))

    def side_slot(u):
        return u if buffers == chunks else lax.rem(u, buffers * pieces)

    def side_sem(s):
        return 0 if buffers == chunks else s

    def side_all(u):
        s = side_slot(u)
        return remote(side_in.at[s], side_in.at[s], side_send.at[side_sem(s)], side_recv.at[s],
                      "gx", lax.rem(gx + 1, n_gx))

    def last_all(v):
        return remote(last_in.at[v], last_in.at[v], last_send, last_recv.at[v], "gy", lax.rem(gy + 1, n_gy))

    def side_copy(u, d):
        peer = lax.rem(gx + d, n_gx)
        s = side_slot(u)
        return remote(side_out.at[s, peer], side_in.at[s, d - 1], side_send.at[side_sem(s)], side_recv.at[s],
                      "gx", peer)

    def last_copy(v, d):
        peer = lax.rem(gy + d, n_gy)
        return remote(last_out.at[v, peer], last_in.at[v, d - 1], last_send, last_recv.at[v],
                      "gy", peer)

    def during(t):
        return (t >= 0) & (t < steps)

    def stage_own(t):
        m, q = t // pieces, lax.rem(t, pieces)

        @pl.when((q == 1 % pieces) & (m + 1 < chunks))
        def _():
            forward(m + 1)

        @pl.when(q == 0)
        def _():
            for d in range(1, n_gx):
                fan_landing(m, d).wait_recv()
            for g in range(n_gx):
                for k in range(slots):
                    current[g, k] = window[m, g, k]

        for i in range(wide):
            c = q * wide + i
            lhs = jnp.concatenate([
                jnp.concatenate([current[g, table[c, g * SUB + j]] for g in range(n_gx)], axis=0)
                for j in range(slots)
            ], axis=1)
            rhs = jnp.concatenate([held[c * slots + j] for j in range(slots)], axis=1)
            own[t, i] = lax.dot_general(lhs, rhs, (((1,), (1,)), ((), ())), preferred_element_type=f32)

    def stage_right(t):
        @pl.when(gz == 0)
        def _():
            right_out[t] = own[t].astype(bf16)

        @pl.when(gz > 0)
        def _():
            right_copy(t).wait_recv()

        @pl.when((gz > 0) & (gz < n_gz - 1))
        def _():
            right_out[t] = (own[t] + right_in[t].astype(f32)).astype(bf16)

        @pl.when(gz < n_gz - 1)
        def _():
            right_copy(t).start()

    def stage_left(t):
        @pl.when(gz == n_gz - 1)
        def _():
            left_out[t] = own[t].astype(bf16)

        @pl.when(gz < n_gz - 1)
        def _():
            left_copy(t).wait_recv()

        @pl.when((gz > 0) & (gz < n_gz - 1))
        def _():
            left_out[t] = (own[t] + left_in[t].astype(f32)).astype(bf16)

        @pl.when(gz > 0)
        def _():
            left_copy(t).start()

    def stage_sum(t):
        parity, q = lax.rem(t // pieces, 2), lax.rem(t, pieces)

        def keep(total):
            square[parity, pl.ds(q * wide, wide)] = total
            rounded[parity, pl.ds(q * wide, wide)] = total.astype(bf16)

        @pl.when(gz == 0)
        def _():
            keep(own[t] + left_in[t].astype(f32))

        @pl.when(gz == n_gz - 1)
        def _():
            keep(own[t] + right_in[t].astype(f32))

        @pl.when((gz > 0) & (gz < n_gz - 1))
        def _():
            keep(own[t] + right_in[t].astype(f32) + left_in[t].astype(f32))

    def stage_second(u):
        parity, q = lax.rem(u // pieces, 2), lax.rem(u, pieces)
        depth = min(slots, rows)
        s = side_slot(u)
        hold = lax.rem(u, SIDE_LAG + 1)
        if buffers < chunks:
            @pl.when((q == 0) & (u >= buffers * pieces))
            def _():
                pl.semaphore_wait(credit, n_gx - 1)

            @pl.when(u >= buffers * pieces)
            def _():
                side_all(u).wait_send()

        for i in range(broad):
            c = q * broad + i
            lhs = jnp.concatenate([rounded[parity, lists[j, c]] for j in range(depth)], axis=1)
            rhs = jnp.concatenate([held[lists[SUB + j, c]] for j in range(depth)], axis=0)
            near = c - gx * rows
            here = (gy == gz) & (near >= 0) & (near < rows)
            near = jnp.clip(near, 0, rows - 1)
            value = (jnp.where(here, 3.0, 0.0) * square[parity, near]
                     - 2.0 * jnp.dot(lhs, rhs, preferred_element_type=f32))
            mine = value[:high]
            for g in range(1, n_gx):
                mine = jnp.where(gx == g, value[g * high:(g + 1) * high], mine)
            product[hold, i] = mine
            for g in range(n_gx):
                side_out[s, g, i] = value[g * high:(g + 1) * high].astype(bf16)
        for d in range(1, n_gx):
            side_copy(u, d).start()

    def stage_mix(v):
        m, q = v // pieces, lax.rem(v, pieces)
        hold = lax.rem(v, SIDE_LAG + 1)
        s = side_slot(v)
        side_all(v).wait_recv()
        for i in range(0, broad, 2):
            pair = []
            for h in range(i, i + 2):
                value = product[hold, h]
                for d in range(1, n_gx):
                    value = value + side_in[s, d - 1, h].astype(f32)
                mixed[h] = value
                pair.append(value)
            for y in range(n_gy):
                last_out[v, y, i // 2] = jnp.concatenate(
                    [value[y * SUB:(y + 1) * SUB] for value in pair], axis=0
                ).astype(bf16)
        for d in range(1, n_gy):
            last_copy(v, d).start()
        if buffers < chunks:
            @pl.when((q == pieces - 1) & (m + buffers < chunks))
            def _():
                for d in range(1, n_gx):
                    pl.semaphore_signal(credit, inc=1, device_id={"gx": lax.rem(gx + d, n_gx)},
                                        device_id_type=MESH)
        down = pl.ds(pl.multiple_of(m * SUB, SUB), SUB)
        for i in range(broad):
            across = pl.ds(pl.multiple_of((q * broad + i) * size, size), size)
            out[down, across] = mixed[i, pl.ds(pl.multiple_of(gy * SUB, SUB), SUB)]

    def stage_last(w):
        m, q = w // pieces, lax.rem(w, pieces)
        last_all(w).wait_recv()
        down = pl.ds(pl.multiple_of(m * SUB, SUB), SUB)
        for i in range(0, broad, 2):
            value = last_in[w, 0, i // 2].astype(f32)
            for d in range(2, n_gy):
                value = value + last_in[w, d - 1, i // 2].astype(f32)
            for h in range(2):
                across = pl.ds(pl.multiple_of((q * broad + i + h) * size, size), size)
                out[down, across] += value[h * SUB:(h + 1) * SUB]

    sum_at = (n_gz - 1) * HOP_LAG
    second_at = sum_at + pieces
    mix_at = second_at + SIDE_LAG
    last_at = mix_at + LAST_LAG

    def slot(s, carry):
        for stage, delay in (
            (stage_own, 0),
            (stage_right, gz * HOP_LAG),
            (stage_left, (n_gz - 1 - gz) * HOP_LAG),
            (stage_sum, sum_at),
            (stage_mix, mix_at),
            (stage_second, second_at),
            (stage_last, last_at),
        ):
            pl.when(during(s - delay))(functools.partial(stage, s - delay))
        return carry

    lax.fori_loop(0, steps + last_at, slot, jnp.int32(0))

    @pl.when(gz < n_gz - 1)
    def _():
        remote(right_out, right_out, right_send, right_recv.at[0], "gz", lax.rem(gz + 1, n_gz)).wait_send()

    @pl.when(gz > 0)
    def _():
        remote(left_out, left_out, left_send, left_recv.at[0], "gz", lax.rem(gz + n_gz - 1, n_gz)).wait_send()

    remote(last_in, last_in, last_send, last_recv.at[0], "gy", lax.rem(gy + 1, n_gy)).wait_send()
    if buffers == chunks:
        remote(side_in, side_in, side_send.at[0], side_recv.at[0], "gx", lax.rem(gx + 1, n_gx)).wait_send()
    else:
        @pl.loop(0, buffers * pieces)
        def _(t):
            side_all(t).wait_send()

    for d in range(1, n_gx):
        head_fan(d).wait_send()
        whole = window.at[:, gx]
        remote(whole, whole, fan_send.at[d - 1], fan_recv.at[0, d - 1], "gx", lax.rem(gx + d, n_gx)).wait_send()

    @pl.when(gy == 0)
    def _():
        for peer in range(1, n_gy):
            head_copy(peer).wait_send()
            whole = window.at[:, gx]
            remote(whole, whole, win_send.at[peer], win_recv.at[0], "gy", peer).wait_send()


def local(block_values, block_cols):
    n_gx, n_gy, n_gz = (lax.axis_size(a) for a in ("gx", "gy", "gz"))
    rows, slots = block_cols.shape[1], block_cols.shape[3]
    size = block_values.shape[4]
    tiles = block_values.reshape(rows * slots, size, size)
    count = n_gx * rows
    chunks = size // (n_gy * SUB)
    high = n_gy * SUB
    pieces = pieces_of(rows, PIECES)
    wide, broad, steps = rows // pieces, count // pieces, chunks * pieces
    tall = n_gx * high
    buffers = chunks if n_gx <= 4 else 2
    top = min(SUB, rows)
    limit = VMEM if buffers < chunks else VMEM - 4 * rows * slots * size * size
    dma = pltpu.SemaphoreType.DMA
    f32, bf16 = jnp.float32, jnp.bfloat16
    flow = (steps, wide, tall, size)
    return pl.pallas_call(
        functools.partial(step_kernel, n_gx, n_gy, n_gz, slots, pieces, buffers),
        out_shape=jax.ShapeDtypeStruct((size // n_gy, count * size), f32),
        in_specs=[pl.BlockSpec(memory_space=pl.ANY), pl.BlockSpec(memory_space=pltpu.VMEM)],
        out_specs=pl.BlockSpec(memory_space=pltpu.VMEM),
        scratch_shapes=[
            pltpu.VMEM((rows * slots, size, size), bf16),
            pltpu.VMEM((chunks, n_gx, slots, high, size), bf16),
            pltpu.VMEM((n_gx, slots + 1, high, size), bf16),
            pltpu.VMEM((n_gx, top, LANES), jnp.int32),
            pltpu.VMEM((rows, LANES), jnp.int32),
            pltpu.VMEM((2 * SUB, LANES), jnp.int32),
            pltpu.SMEM((rows, LANES), jnp.int32),
            pltpu.SMEM((2 * SUB, LANES), jnp.int32),
            pltpu.VMEM(flow, f32),
            pltpu.VMEM(flow, bf16), pltpu.VMEM(flow, bf16), pltpu.VMEM(flow, bf16), pltpu.VMEM(flow, bf16),
            pltpu.VMEM((2, rows, tall, size), f32),
            pltpu.VMEM((2, rows + 1, tall, size), bf16),
            pltpu.VMEM((SIDE_LAG + 1, broad, high, size), f32),
            pltpu.VMEM((buffers * pieces, n_gx, broad, high, size), bf16),
            pltpu.VMEM((buffers * pieces, n_gx - 1, broad, high, size), bf16),
            pltpu.VMEM((broad, high, size), f32),
            pltpu.VMEM((steps, n_gy, broad // 2, 2 * SUB, size), bf16),
            pltpu.VMEM((steps, n_gy - 1, broad // 2, 2 * SUB, size), bf16),
            dma((1 + min(4, rows - 1),)), dma((2, n_gy)), dma((2, n_gx - 1)),
            dma((n_gy,)), dma((chunks,)), dma((n_gx - 1,)), dma((chunks, n_gx - 1)), dma((2,)),
            dma, dma, dma((steps,)), dma((steps,)),
            dma((1 if buffers == chunks else buffers * pieces,)), dma((buffers * pieces,)),
            dma, dma((steps,)),
            pltpu.SemaphoreType.REGULAR,
        ],
        compiler_params=pltpu.CompilerParams(
            collective_id=0, has_side_effects=True, vmem_limit_bytes=limit
        ),
        name="purify",
    )(tiles, jnp.transpose(block_cols, (0, 3, 2, 1)))


def solution(mesh):
    in_specs = (P("gy", "gx", "gz", None, None, None), P("gy", "gx", "gz", None))
    out_specs = P(("gx", "gy"), "gz")
    return jax.shard_map(local, mesh=mesh, in_specs=in_specs, out_specs=out_specs, check_vma=False)
```

```python
import functools

import jax
import jax.numpy as jnp
from jax import lax
from jax.experimental import pallas as pl
from jax.experimental.pallas import tpu as pltpu
from jax.sharding import PartitionSpec as P

LANES = 128
SUB = 8
VMEM = 67043328
MESH = pl.DeviceIdType.MESH
HOP_LAG, SIDE_LAG, LAST_LAG = 3, 2, 6
SEED_HOP, TURN_AT, TURN_LAST, JOIN_LAG, COLLECT_LAG, PASS_LAG, END_LAG = 2, 6, 6, 4, 2, 4, 5
PIECES = 8


def pieces_of(count, most):
    for pieces in range(min(count, most), 0, -1):
        if count % pieces == 0:
            return pieces


def greet(axes, plane):
    barrier = pltpu.get_barrier_semaphore()
    total = 0
    for axis in axes:
        size = lax.axis_size(axis)
        me = lax.axis_index(axis)
        for step in range(1, size):
            pl.semaphore_signal(
                barrier, inc=1, device_id={axis: lax.rem(me + step, size)}, device_id_type=MESH
            )
        total += size - 1
    if plane:
        n_gx, n_gy = lax.axis_size("gx"), lax.axis_size("gy")
        for dx in range(1, n_gx):
            for dy in range(1, n_gy):
                peer = {"gx": lax.rem(lax.axis_index("gx") + dx, n_gx),
                        "gy": lax.rem(lax.axis_index("gy") + dy, n_gy)}
                pl.semaphore_signal(barrier, inc=1, device_id=peer, device_id_type=MESH)
        total += (n_gx - 1) * (n_gy - 1)
    pl.semaphore_wait(barrier, total)


def remote(src, dst, send, recv, axis, peer):
    return pltpu.make_async_remote_copy(
        src_ref=src, dst_ref=dst, send_sem=send, recv_sem=recv,
        device_id={axis: peer}, device_id_type=MESH,
    )


def step_kernel(
    n_gx, n_gy, n_gz, slots, pieces, buffers, twos,
    tiles, cols, out,
    held, window, current, heads, table_v, lists_v, table, lists,
    own, right_out, left_out, right_in, left_in, square, rounded,
    product, side_out, side_in, mixed, last_out, last_in,
    load_sem, head_sem, head_side, win_send, win_recv, fan_send, fan_recv, table_sem,
    right_send, left_send, right_recv, left_recv, side_send, side_recv, last_send, last_recv, credit,
    *more,
):
    gx, gy, gz = lax.axis_index("gx"), lax.axis_index("gy"), lax.axis_index("gz")
    rows = cols.shape[3]
    size = tiles.shape[2]
    count = n_gx * rows
    chunks = window.shape[0]
    block = size // n_gy
    high = n_gy * SUB
    wide = rows // pieces
    broad = count // pieces
    steps = chunks * pieces
    f32, bf16 = jnp.float32, jnp.bfloat16

    first_load = pltpu.make_async_copy(tiles.at[pl.ds(0, slots)], held.at[pl.ds(0, slots)], load_sem.at[0])
    first_load.start()
    loads = [first_load]
    parts = load_sem.shape[0] - 1
    for part in range(parts):
        low, top = 1 + (rows - 1) * part // parts, 1 + (rows - 1) * (part + 1) // parts
        loads.append(pltpu.make_async_copy(
            tiles.at[pl.ds(low * slots, (top - low) * slots)], held.at[pl.ds(low * slots, (top - low) * slots)],
            load_sem.at[part + 1],
        ))
        loads[-1].start()
    greet(("gx", "gy", "gz"), twos > 0)

    def win_copy(m, peer):
        return remote(window.at[m, gx], window.at[m, gx], win_send.at[peer], win_recv.at[m], "gy", peer)

    def fan_copy(m, d):
        return remote(window.at[m, gx], window.at[m, gx], fan_send.at[d - 1], fan_recv.at[m, d - 1],
                      "gx", lax.rem(gx + d, n_gx))

    def fan_landing(m, d):
        g = lax.rem(gx - d + n_gx, n_gx)
        return remote(window.at[m, g], window.at[m, g], fan_send.at[d - 1], fan_recv.at[m, d - 1],
                      "gx", lax.rem(gx + d, n_gx))

    def head_copy(peer):
        return remote(heads.at[gx], heads.at[gx], head_sem.at[0, peer], head_sem.at[1, 0], "gy", peer)

    def head_fan(d):
        return remote(heads.at[gx], heads.at[gx], head_side.at[0, d - 1], head_side.at[1, d - 1],
                      "gx", lax.rem(gx + d, n_gx))

    def head_landing(d):
        g = lax.rem(gx - d + n_gx, n_gx)
        return remote(heads.at[g], heads.at[g], head_side.at[0, d - 1], head_side.at[1, d - 1],
                      "gx", lax.rem(gx + d, n_gx))

    lanes = lax.broadcasted_iota(jnp.int32, (rows, LANES), 1)
    places = lax.broadcasted_iota(jnp.int32, (rows, LANES), 0)
    listed = cols[0, :, 0, :].T
    each = [jnp.broadcast_to(listed[:, k:k + 1], (rows, LANES)) for k in range(slots)]
    spread = jnp.full((rows, LANES), -1, jnp.int32)
    for k in range(slots):
        spread = jnp.where(lanes == k, each[k], spread)

    @pl.when(gy == 0)
    def _():
        heads[gx] = spread[:heads.shape[1]]
        for peer in range(1, n_gy):
            head_copy(peer).start()
        for d in range(1, n_gx):
            head_fan(d).start()
        first_load.wait()
        for k in range(slots):
            tile = held[k].astype(f32)
            for m in range(chunks):
                window[m, gx, k] = jnp.concatenate(
                    [tile[q * block + m * SUB:][:SUB] for q in range(n_gy)], axis=0
                ).astype(bf16)
        for m in range(chunks):
            for peer in range(1, n_gy):
                win_copy(m, peer).start()
            for d in range(1, n_gx):
                fan_copy(m, d).start()

    marks = [jnp.where(each[k] == lanes, places * SUB + k, -1) for k in range(slots)]
    lists_v[...] = jnp.zeros_like(lists_v)
    for i in range(slots):
        top = marks[0]
        for k in range(1, slots):
            top = jnp.maximum(top, marks[k])
        top = jnp.max(top, axis=0, keepdims=True)
        marks = [jnp.where(mark == top, -1, mark) for mark in marks]
        row, slot = top // SUB, top % SUB
        lists_v[i:i + 1] = jnp.where(top < 0, rows, row)
        lists_v[SUB + i:SUB + i + 1] = jnp.where(top < 0, 0, row * slots + slot)
    list_copy = pltpu.make_async_copy(lists_v, lists, table_sem.at[0])
    list_copy.start()
    for load in loads[1:]:
        load.wait()

    @pl.when(gy != 0)
    def _():
        first_load.wait()

    list_copy.wait()
    if twos:
        (seed, ids, lists2_v, lists2, listed_v, listed_s, product2, mixed2, side2_out, side2_in,
         last2_out, last2_in, gat, s2_out, s2_in, full, r_out, r_in, z_in,
         seed_send, seed_recv, ids_send, ids_recv, table2_sem, side2_send, side2_recv, last2_send, last2_recv,
         gat_send, gat_recv, s2_send, s2_recv, r_send, r_recv, z_send, z_recv) = more
        tall2 = twos * SUB
        high2 = n_gy * tall2
        down2 = pl.ds(block - tall2, tall2)
        plane = n_gy * n_gx
        me = gy * n_gx + gx
        seeds = seed_recv.shape[0]
        each_seed = slots // seeds
        listed_v[...] = spread
        listed_copy = pltpu.make_async_copy(listed_v, listed_s, table2_sem.at[0])
        listed_copy.start()
        seed[slots] = jnp.zeros((n_gx, high2, size), bf16)

        def seed_copy(p):
            part = seed.at[pl.ds(p * each_seed, each_seed)]
            return remote(part, part, seed_send, seed_recv.at[p], "gz", lax.rem(gz + 1, n_gz))

        def ids_copy(peer):
            return remote(lists_v.at[pl.ds(0, SUB)], ids, ids_send.at[peer], ids_recv, "gz", peer)

        @pl.when(gz == 0)
        def _():
            for peer in range(1, n_gz):
                ids_copy(peer).start()
            ids[...] = lists_v[0:SUB]
            across = lax.broadcasted_iota(jnp.int32, (high2, size), 1)
            at = lax.broadcasted_iota(jnp.int32, (high2, size), 0)
            pick = (at // tall2) * block + (block - tall2) + at % tall2
            pick = jnp.where(across == pick, 1.0, 0.0).astype(bf16)
            for p in range(seeds):
                for i in range(p * each_seed, (p + 1) * each_seed):
                    for g in range(n_gx):
                        tile = held[lists[SUB + i, g * rows]]
                        seed[i, g] = lax.dot_general(
                            pick, tile, (((1,), (1,)), ((), ())), preferred_element_type=f32
                        ).astype(bf16)
                seed_copy(p).start()

    for g in range(n_gx):
        current[g, slots] = jnp.zeros((high, size), bf16)
    for parity in range(2):
        rounded[parity, rows] = jnp.zeros((n_gx * high, size), bf16)

    @pl.when(gy != 0)
    def _():
        head_copy(0).wait_recv()
        for d in range(1, n_gx):
            head_fan(d).start()

    for d in range(1, n_gx):
        head_landing(d).wait_recv()
    total = jnp.zeros((rows, LANES), jnp.int32)
    for g in range(n_gx):
        found = jnp.full((rows, LANES), slots, jnp.int32)
        for k in range(slots):
            found = jnp.where(spread == jnp.broadcast_to(heads[g, 0:1, k:k + 1], (rows, LANES)), k, found)
        found = jnp.where(lanes < slots, found, 0)
        total = total + (found if g == 0 else pltpu.roll(found, g * SUB, 1))
    table_v[...] = total
    table_copy = pltpu.make_async_copy(table_v, table, table_sem.at[1])
    table_copy.start()

    def forward(m):
        @pl.when(gy != 0)
        def _():
            win_copy(m, 0).wait_recv()
            for d in range(1, n_gx):
                fan_copy(m, d).start()

    forward(0)
    table_copy.wait()
    if twos:
        @pl.when(gz > 0)
        def _():
            ids_copy(0).wait_recv()

        mine = lists_v[0:SUB]
        for g in range(n_gx):
            found = jnp.full((SUB, LANES), slots, jnp.int32)
            for j in range(slots):
                label = jnp.broadcast_to(ids[j:j + 1, g * rows:g * rows + 1], (SUB, LANES))
                found = jnp.where(mine == label, j, found)
            lists2_v[g * SUB:(g + 1) * SUB] = jnp.where(mine >= rows, slots, found)
        lists2_copy = pltpu.make_async_copy(lists2_v, lists2, table2_sem.at[1])
        lists2_copy.start()
        listed_copy.wait()
        lists2_copy.wait()

    def right_copy(t):
        return remote(right_out.at[t], right_in.at[t], right_send, right_recv.at[t],
                      "gz", lax.rem(gz + 1, n_gz))

    def left_copy(t):
        return remote(left_out.at[t], left_in.at[t], left_send, left_recv.at[t],
                      "gz", lax.rem(gz + n_gz - 1, n_gz))

    def side_slot(u):
        return u if buffers == chunks else lax.rem(u, buffers * pieces)

    def side_sem(s):
        return 0 if buffers == chunks else s

    def side_all(u):
        s = side_slot(u)
        return remote(side_in.at[s], side_in.at[s], side_send.at[side_sem(s)], side_recv.at[s],
                      "gx", lax.rem(gx + 1, n_gx))

    def last_all(v):
        return remote(last_in.at[v], last_in.at[v], last_send, last_recv.at[v], "gy", lax.rem(gy + 1, n_gy))

    def side_copy(u, d):
        peer = lax.rem(gx + d, n_gx)
        s = side_slot(u)
        return remote(side_out.at[s, peer], side_in.at[s, d - 1], side_send.at[side_sem(s)], side_recv.at[s],
                      "gx", peer)

    def last_copy(v, d):
        peer = lax.rem(gy + d, n_gy)
        return remote(last_out.at[v, peer], last_in.at[v, d - 1], last_send, last_recv.at[v],
                      "gy", peer)

    def stage_own(t):
        m, q = t // pieces, lax.rem(t, pieces)

        @pl.when((q == 1 % pieces) & (m + 1 < chunks))
        def _():
            forward(m + 1)

        @pl.when(q == 0)
        def _():
            for d in range(1, n_gx):
                fan_landing(m, d).wait_recv()
            for g in range(n_gx):
                for k in range(slots):
                    current[g, k] = window[m, g, k]

        for i in range(wide):
            c = q * wide + i
            lhs = jnp.concatenate([
                jnp.concatenate([current[g, table[c, g * SUB + j]] for g in range(n_gx)], axis=0)
                for j in range(slots)
            ], axis=1)
            rhs = jnp.concatenate([held[c * slots + j] for j in range(slots)], axis=1)
            own[t, i] = lax.dot_general(lhs, rhs, (((1,), (1,)), ((), ())), preferred_element_type=f32)

    def stage_right(t):
        @pl.when(gz == 0)
        def _():
            right_out[t] = own[t].astype(bf16)

        @pl.when(gz > 0)
        def _():
            right_copy(t).wait_recv()

        @pl.when((gz > 0) & (gz < n_gz - 1))
        def _():
            right_out[t] = (own[t] + right_in[t].astype(f32)).astype(bf16)

        @pl.when(gz < n_gz - 1)
        def _():
            right_copy(t).start()

    def stage_left(t):
        @pl.when(gz == n_gz - 1)
        def _():
            left_out[t] = own[t].astype(bf16)

        @pl.when(gz < n_gz - 1)
        def _():
            left_copy(t).wait_recv()

        @pl.when((gz > 0) & (gz < n_gz - 1))
        def _():
            left_out[t] = (own[t] + left_in[t].astype(f32)).astype(bf16)

        @pl.when(gz > 0)
        def _():
            left_copy(t).start()

    def stage_sum(t):
        parity, q = lax.rem(t // pieces, 2), lax.rem(t, pieces)

        def keep(total):
            square[parity, pl.ds(q * wide, wide)] = total
            rounded[parity, pl.ds(q * wide, wide)] = total.astype(bf16)

        @pl.when(gz == 0)
        def _():
            keep(own[t] + left_in[t].astype(f32))

        @pl.when(gz == n_gz - 1)
        def _():
            keep(own[t] + right_in[t].astype(f32))

        @pl.when((gz > 0) & (gz < n_gz - 1))
        def _():
            keep(own[t] + right_in[t].astype(f32) + left_in[t].astype(f32))

    def stage_second(u):
        parity, q = lax.rem(u // pieces, 2), lax.rem(u, pieces)
        depth = min(slots, rows)
        s = side_slot(u)
        hold = lax.rem(u, SIDE_LAG + 1)
        if buffers < chunks:
            @pl.when((q == 0) & (u >= buffers * pieces))
            def _():
                pl.semaphore_wait(credit, n_gx - 1)

            @pl.when(u >= buffers * pieces)
            def _():
                side_all(u).wait_send()

        for i in range(broad):
            c = q * broad + i
            lhs = jnp.concatenate([rounded[parity, lists[j, c]] for j in range(depth)], axis=1)
            rhs = jnp.concatenate([held[lists[SUB + j, c]] for j in range(depth)], axis=0)
            near = c - gx * rows
            here = (gy == gz) & (near >= 0) & (near < rows)
            near = jnp.clip(near, 0, rows - 1)
            value = (jnp.where(here, 3.0, 0.0) * square[parity, near]
                     - 2.0 * jnp.dot(lhs, rhs, preferred_element_type=f32))
            mine = value[:high]
            for g in range(1, n_gx):
                mine = jnp.where(gx == g, value[g * high:(g + 1) * high], mine)
            product[hold, i] = mine
            for g in range(n_gx):
                side_out[s, g, i] = value[g * high:(g + 1) * high].astype(bf16)
        for d in range(1, n_gx):
            side_copy(u, d).start()

    def stage_mix(v):
        m, q = v // pieces, lax.rem(v, pieces)
        hold = lax.rem(v, SIDE_LAG + 1)
        s = side_slot(v)
        side_all(v).wait_recv()
        for i in range(0, broad, 2):
            pair = []
            for h in range(i, i + 2):
                value = product[hold, h]
                for d in range(1, n_gx):
                    value = value + side_in[s, d - 1, h].astype(f32)
                mixed[h] = value
                pair.append(value)
            for y in range(n_gy):
                last_out[v, y, i // 2] = jnp.concatenate(
                    [value[y * SUB:(y + 1) * SUB] for value in pair], axis=0
                ).astype(bf16)
        for d in range(1, n_gy):
            last_copy(v, d).start()
        if buffers < chunks:
            @pl.when((q == pieces - 1) & (m + buffers < chunks))
            def _():
                for d in range(1, n_gx):
                    pl.semaphore_signal(credit, inc=1, device_id={"gx": lax.rem(gx + d, n_gx)},
                                        device_id_type=MESH)
        down = pl.ds(pl.multiple_of(m * SUB, SUB), SUB)
        for i in range(broad):
            across = pl.ds(pl.multiple_of((q * broad + i) * size, size), size)
            out[down, across] = mixed[i, pl.ds(pl.multiple_of(gy * SUB, SUB), SUB)]

    def stage_last(w):
        m, q = w // pieces, lax.rem(w, pieces)
        last_all(w).wait_recv()
        down = pl.ds(pl.multiple_of(m * SUB, SUB), SUB)
        for i in range(0, broad, 2):
            value = last_in[w, 0, i // 2].astype(f32)
            for d in range(2, n_gy):
                value = value + last_in[w, d - 1, i // 2].astype(f32)
            for h in range(2):
                across = pl.ds(pl.multiple_of((q * broad + i + h) * size, size), size)
                out[down, across] += value[h * SUB:(h + 1) * SUB]

    def pass_seed(p):
        @pl.when(gz > 0)
        def _():
            seed_copy(p).wait_recv()

        @pl.when((gz > 0) & (gz < n_gz - 1))
        def _():
            seed_copy(p).start()

    def across_of(c):
        return pl.ds(pl.multiple_of(c * size, size), size)

    def side2_copy(q, d):
        peer = lax.rem(gx + d, n_gx)
        return remote(side2_out.at[q, peer], side2_in.at[q, d - 1], side2_send, side2_recv.at[q], "gx", peer)

    def last2_copy(q, d):
        peer = lax.rem(gy + d, n_gy)
        return remote(last2_out.at[q, peer], last2_in.at[q, d - 1], last2_send, last2_recv.at[q], "gy", peer)

    def gat_copy(q, d):
        return remote(gat.at[q, 0], gat.at[q, d], gat_send, gat_recv.at[q], "gy", lax.rem(gy + d, n_gy))

    def s2_copy(q, d):
        return remote(s2_out.at[q], s2_in.at[q, d - 1], s2_send, s2_recv.at[q], "gx", lax.rem(gx + d, n_gx))

    def wait_all(ref, send, recv):
        remote(ref, ref, send, recv, "gy", lax.rem(gy + 1, n_gy)).wait_recv()

    def turn_first(q):
        hold = lax.rem(q, SIDE_LAG + 1)
        depth = min(slots, rows)
        for i in range(broad):
            c = q * broad + i
            lhs = jnp.concatenate([
                jnp.concatenate([seed[lists2[g * SUB + j, c], g] for g in range(n_gx)], axis=0)
                for j in range(depth)
            ], axis=1)
            rhs = jnp.concatenate([held[lists[SUB + j, c]] for j in range(depth)], axis=0)
            value = jnp.dot(lhs, rhs, preferred_element_type=f32)
            mine = value[:high2]
            for g in range(1, n_gx):
                mine = jnp.where(gx == g, value[g * high2:(g + 1) * high2], mine)
            product2[hold, i] = mine
            for g in range(n_gx):
                side2_out[q, g, i] = value[g * high2:(g + 1) * high2].astype(bf16)
        for d in range(1, n_gx):
            side2_copy(q, d).start()

    def turn_mix(q):
        hold = lax.rem(q, SIDE_LAG + 1)
        wait_all(side2_in.at[q], side2_send, side2_recv.at[q])
        for i in range(broad):
            value = product2[hold, i]
            for d in range(1, n_gx):
                value = value + side2_in[q, d - 1, i].astype(f32)
            mixed2[i] = value
            for y in range(n_gy):
                last2_out[q, y, i] = value[y * tall2:(y + 1) * tall2].astype(bf16)
        for d in range(1, n_gy):
            last2_copy(q, d).start()
        for i in range(broad):
            out[down2, across_of(q * broad + i)] = mixed2[i, pl.ds(pl.multiple_of(gy * tall2, tall2), tall2)]

    def turn_last(q):
        wait_all(last2_in.at[q], last2_send, last2_recv.at[q])
        for i in range(broad):
            total = out[down2, across_of(q * broad + i)]
            for d in range(1, n_gy):
                total = total + last2_in[q, d - 1, i].astype(f32)
            gat[q, 0, i] = total.astype(bf16)
            out[down2, across_of(q * broad + i)] = 3.0 * total
        for d in range(1, n_gy):
            gat_copy(q, d).start()

    def turn_join(q):
        wait_all(gat.at[q, pl.ds(1, n_gy - 1)], gat_send, gat_recv.at[q])
        for i in range(broad):
            tile = jnp.concatenate([gat[q, lax.rem(gy - y + n_gy, n_gy), i] for y in range(n_gy)], axis=0)
            s2_out[q, i] = tile
            full[gx, q * broad + i] = tile
        for d in range(1, n_gx):
            s2_copy(q, d).start()

    def turn_collect(q):
        wait_all(s2_in.at[q], s2_send, s2_recv.at[q])
        for d in range(1, n_gx):
            g = lax.rem(gx - d + n_gx, n_gx)
            full[g, pl.ds(q * broad, broad)] = s2_in[q, d - 1]

    def turn_back(q):
        for i in range(wide):
            c = q * wide + i
            lhs = jnp.concatenate([
                jnp.concatenate([full[g, listed_s[c, j]] for g in range(n_gx)], axis=0)
                for j in range(slots)
            ], axis=1)
            rhs = jnp.concatenate([held[c * slots + j] for j in range(slots)], axis=1)
            value = -2.0 * lax.dot_general(lhs, rhs, (((1,), (1,)), ((), ())), preferred_element_type=f32)
            for g in range(n_gx):
                for y in range(n_gy):
                    low = g * high2 + y * tall2
                    r_out[q, y * n_gx + g, i] = value[low:low + tall2].astype(bf16)
        for d in range(1, plane):
            peer = lax.rem(me + d, plane)
            pltpu.make_async_remote_copy(
                src_ref=r_out.at[q, peer], dst_ref=r_in.at[q, plane - d], send_sem=r_send, recv_sem=r_recv.at[q],
                device_id={"gx": lax.rem(peer, n_gx), "gy": peer // n_gx}, device_id_type=MESH,
            ).start()
        r_in[q, 0] = r_out[q, me]

    def from_slab(a, x):
        return lax.rem(a * n_gx + x - me + plane, plane)

    def turn_pass(q):
        wait_all(r_in.at[q, pl.ds(1, plane - 1)], r_send, r_recv.at[q])
        for d in range(1, n_gz):
            a = lax.rem(gz + d, n_gz)
            for x in range(n_gx):
                remote(r_in.at[q, from_slab(a, x)], z_in.at[q, d - 1, x], z_send, z_recv.at[q], "gz", a).start()

    def turn_end(q):
        wait_all(z_in.at[q], z_send, z_recv.at[q])
        for x in range(n_gx):
            for i in range(wide):
                value = r_in[q, from_slab(gz, x), i].astype(f32)
                for d in range(1, n_gz):
                    value = value + z_in[q, d - 1, x, i].astype(f32)
                out[down2, across_of(x * rows + q * wide + i)] += value

    sum_at = (n_gz - 1) * HOP_LAG
    second_at = sum_at + pieces
    mix_at = second_at + SIDE_LAG
    last_at = mix_at + LAST_LAG

    stages = [
        (stage_own, 0, steps),
        (stage_right, gz * HOP_LAG, steps),
        (stage_left, (n_gz - 1 - gz) * HOP_LAG, steps),
        (stage_sum, sum_at, steps),
        (stage_mix, mix_at, steps),
        (stage_second, second_at, steps),
        (stage_last, last_at, steps),
    ]
    slots_needed = steps + last_at
    if twos:
        turn_mix_at = TURN_AT + SIDE_LAG
        turn_last_at = turn_mix_at + TURN_LAST
        join_at = turn_last_at + JOIN_LAG
        collect_at = join_at + COLLECT_LAG
        back_at = collect_at + pieces
        pass_at = back_at + PASS_LAG
        end_at = pass_at + END_LAG
        stages = stages[:4] + [
            (pass_seed, (gz - 1) * SEED_HOP, seeds),
            (stage_mix, mix_at, steps),
            (turn_mix, turn_mix_at, pieces),
            (turn_pass, pass_at, pieces),
            (turn_back, back_at, pieces),
            (stage_second, second_at, steps),
            (turn_first, TURN_AT, pieces),
            (stage_last, last_at, steps),
            (turn_last, turn_last_at, pieces),
            (turn_join, join_at, pieces),
            (turn_collect, collect_at, pieces),
            (turn_end, end_at, pieces),
        ]
        slots_needed = max(slots_needed, end_at + pieces)

    def slot(s, carry):
        for stage, delay, span in stages:
            t = s - delay
            pl.when((t >= 0) & (t < span))(functools.partial(stage, t))
        return carry

    lax.fori_loop(0, slots_needed, slot, jnp.int32(0))

    @pl.when(gz < n_gz - 1)
    def _():
        remote(right_out, right_out, right_send, right_recv.at[0], "gz", lax.rem(gz + 1, n_gz)).wait_send()

    @pl.when(gz > 0)
    def _():
        remote(left_out, left_out, left_send, left_recv.at[0], "gz", lax.rem(gz + n_gz - 1, n_gz)).wait_send()

    remote(last_in, last_in, last_send, last_recv.at[0], "gy", lax.rem(gy + 1, n_gy)).wait_send()
    if buffers == chunks:
        remote(side_in, side_in, side_send.at[0], side_recv.at[0], "gx", lax.rem(gx + 1, n_gx)).wait_send()
    else:
        @pl.loop(0, buffers * pieces)
        def _(t):
            side_all(t).wait_send()

    if twos:
        def sent(ref, send, recv):
            remote(ref, ref, send, recv, "gy", lax.rem(gy + 1, n_gy)).wait_send()

        sent(side2_in, side2_send, side2_recv.at[0])
        sent(last2_in, last2_send, last2_recv.at[0])
        sent(gat.at[:, pl.ds(1, n_gy - 1)], gat_send, gat_recv.at[0])
        sent(s2_in, s2_send, s2_recv.at[0])
        sent(r_in.at[:, pl.ds(1, plane - 1)], r_send, r_recv.at[0])
        sent(z_in, z_send, z_recv.at[0])

        @pl.when(gz < n_gz - 1)
        def _():
            sent(seed.at[pl.ds(0, slots)], seed_send, seed_recv.at[0])

        @pl.when(gz == 0)
        def _():
            for peer in range(1, n_gz):
                ids_copy(peer).wait_send()

    for d in range(1, n_gx):
        head_fan(d).wait_send()
        whole = window.at[:, gx]
        remote(whole, whole, fan_send.at[d - 1], fan_recv.at[0, d - 1], "gx", lax.rem(gx + d, n_gx)).wait_send()

    @pl.when(gy == 0)
    def _():
        for peer in range(1, n_gy):
            head_copy(peer).wait_send()
            whole = window.at[:, gx]
            remote(whole, whole, win_send.at[peer], win_recv.at[0], "gy", peer).wait_send()


def local(block_values, block_cols):
    n_gx, n_gy, n_gz = (lax.axis_size(a) for a in ("gx", "gy", "gz"))
    rows, slots = block_cols.shape[1], block_cols.shape[3]
    size = block_values.shape[4]
    tiles = block_values.reshape(rows * slots, size, size)
    count = n_gx * rows
    chunks = size // (n_gy * SUB)
    twos = 1 if n_gx <= 4 and chunks > 2 and n_gy == n_gz else 0
    chunks = chunks - twos
    high = n_gy * SUB
    pieces = pieces_of(rows, PIECES)
    wide, broad, steps = rows // pieces, count // pieces, chunks * pieces
    tall = n_gx * high
    buffers = chunks if n_gx <= 4 else 2
    top = min(SUB, rows)
    limit = VMEM if buffers < chunks else VMEM - 4 * rows * slots * size * size
    dma = pltpu.SemaphoreType.DMA
    f32, bf16 = jnp.float32, jnp.bfloat16
    flow = (steps, wide, tall, size)
    more = []
    if twos:
        tall2 = twos * SUB
        high2, plane, seeds = n_gy * tall2, n_gy * n_gx, pieces_of(slots, 3)
        more = [
            pltpu.VMEM((slots + 1, n_gx, high2, size), bf16),
            pltpu.VMEM((SUB, LANES), jnp.int32),
            pltpu.VMEM((n_gx * SUB, LANES), jnp.int32),
            pltpu.SMEM((n_gx * SUB, LANES), jnp.int32),
            pltpu.VMEM((rows, LANES), jnp.int32),
            pltpu.SMEM((rows, LANES), jnp.int32),
            pltpu.VMEM((SIDE_LAG + 1, broad, high2, size), f32),
            pltpu.VMEM((broad, high2, size), f32),
            pltpu.VMEM((pieces, n_gx, broad, high2, size), bf16),
            pltpu.VMEM((pieces, n_gx - 1, broad, high2, size), bf16),
            pltpu.VMEM((pieces, n_gy, broad, tall2, size), bf16),
            pltpu.VMEM((pieces, n_gy - 1, broad, tall2, size), bf16),
            pltpu.VMEM((pieces, n_gy, broad, tall2, size), bf16),
            pltpu.VMEM((pieces, broad, high2, size), bf16),
            pltpu.VMEM((pieces, n_gx - 1, broad, high2, size), bf16),
            pltpu.VMEM((n_gx, count, high2, size), bf16),
            pltpu.VMEM((pieces, plane, wide, tall2, size), bf16),
            pltpu.VMEM((pieces, plane, wide, tall2, size), bf16),
            pltpu.VMEM((pieces, n_gz - 1, n_gx, wide, tall2, size), bf16),
            dma, dma((seeds,)), dma((n_gz,)), dma, dma((2,)),
            dma, dma((pieces,)), dma, dma((pieces,)), dma, dma((pieces,)),
            dma, dma((pieces,)), dma, dma((pieces,)), dma, dma((pieces,)),
        ]
    return pl.pallas_call(
        functools.partial(step_kernel, n_gx, n_gy, n_gz, slots, pieces, buffers, twos),
        out_shape=jax.ShapeDtypeStruct((size // n_gy, count * size), f32),
        in_specs=[pl.BlockSpec(memory_space=pl.ANY), pl.BlockSpec(memory_space=pltpu.VMEM)],
        out_specs=pl.BlockSpec(memory_space=pltpu.VMEM),
        scratch_shapes=[
            pltpu.VMEM((rows * slots, size, size), bf16),
            pltpu.VMEM((chunks, n_gx, slots, high, size), bf16),
            pltpu.VMEM((n_gx, slots + 1, high, size), bf16),
            pltpu.VMEM((n_gx, top, LANES), jnp.int32),
            pltpu.VMEM((rows, LANES), jnp.int32),
            pltpu.VMEM((2 * SUB, LANES), jnp.int32),
            pltpu.SMEM((rows, LANES), jnp.int32),
            pltpu.SMEM((2 * SUB, LANES), jnp.int32),
            pltpu.VMEM(flow, f32),
            pltpu.VMEM(flow, bf16), pltpu.VMEM(flow, bf16), pltpu.VMEM(flow, bf16), pltpu.VMEM(flow, bf16),
            pltpu.VMEM((2, rows, tall, size), f32),
            pltpu.VMEM((2, rows + 1, tall, size), bf16),
            pltpu.VMEM((SIDE_LAG + 1, broad, high, size), f32),
            pltpu.VMEM((buffers * pieces, n_gx, broad, high, size), bf16),
            pltpu.VMEM((buffers * pieces, n_gx - 1, broad, high, size), bf16),
            pltpu.VMEM((broad, high, size), f32),
            pltpu.VMEM((steps, n_gy, broad // 2, 2 * SUB, size), bf16),
            pltpu.VMEM((steps, n_gy - 1, broad // 2, 2 * SUB, size), bf16),
            dma((1 + min(4, rows - 1),)), dma((2, n_gy)), dma((2, n_gx - 1)),
            dma((n_gy,)), dma((chunks,)), dma((n_gx - 1,)), dma((chunks, n_gx - 1)), dma((2,)),
            dma, dma, dma((steps,)), dma((steps,)),
            dma((1 if buffers == chunks else buffers * pieces,)), dma((buffers * pieces,)),
            dma, dma((steps,)),
            pltpu.SemaphoreType.REGULAR,
        ] + more,
        compiler_params=pltpu.CompilerParams(
            collective_id=0, has_side_effects=True, vmem_limit_bytes=limit
        ),
        name="purify",
    )(tiles, jnp.transpose(block_cols, (0, 3, 2, 1)))


def solution(mesh):
    in_specs = (P("gy", "gx", "gz", None, None, None), P("gy", "gx", "gz", None))
    out_specs = P(("gx", "gy"), "gz")
    return jax.shard_map(local, mesh=mesh, in_specs=in_specs, out_specs=out_specs, check_vma=False)
```

```python
import functools

import jax
import jax.numpy as jnp
from jax import lax
from jax.experimental import pallas as pl
from jax.experimental.pallas import tpu as pltpu
from jax.sharding import PartitionSpec as P

LANES = 128
SUB = 8
VMEM = 67043328
MESH = pl.DeviceIdType.MESH
HOP_LAG, SIDE_LAG, LAST_LAG = 6, 2, 6
SEED_HOP, TURN_AT, TURN_LAST, JOIN_LAG, COLLECT_LAG, PASS_LAG, END_LAG = 2, 6, 6, 4, 2, 5, 7
PIECES, GROUPS = 8, 4


def pieces_of(count, most):
    for pieces in range(min(count, most), 0, -1):
        if count % pieces == 0:
            return pieces


def knock(axes, plane):
    barrier = pltpu.get_barrier_semaphore()
    total = 0
    for axis in axes:
        size = lax.axis_size(axis)
        me = lax.axis_index(axis)
        for step in range(1, size):
            pl.semaphore_signal(
                barrier, inc=1, device_id={axis: lax.rem(me + step, size)}, device_id_type=MESH
            )
        total += size - 1
    if plane:
        n_gx, n_gy = lax.axis_size("gx"), lax.axis_size("gy")
        for dx in range(1, n_gx):
            for dy in range(1, n_gy):
                peer = {"gx": lax.rem(lax.axis_index("gx") + dx, n_gx),
                        "gy": lax.rem(lax.axis_index("gy") + dy, n_gy)}
                pl.semaphore_signal(barrier, inc=1, device_id=peer, device_id_type=MESH)
        total += (n_gx - 1) * (n_gy - 1)
    return lambda: pl.semaphore_wait(barrier, total)


def remote(src, dst, send, recv, axis, peer):
    return pltpu.make_async_remote_copy(
        src_ref=src, dst_ref=dst, send_sem=send, recv_sem=recv,
        device_id={axis: peer}, device_id_type=MESH,
    )


def step_kernel(
    n_gx, n_gy, n_gz, slots, pieces, buffers, twos,
    tiles, cols, out,
    held, window, current, heads, table_v, lists_v, table, lists,
    own, right_out, left_out, right_in, left_in, square, rounded,
    product, side_out, side_in, mixed, last_out, last_in,
    load_sem, head_sem, head_side, win_send, win_recv, fan_send, fan_recv, table_sem,
    right_send, left_send, right_recv, left_recv, side_send, side_recv, last_send, last_recv, credit,
    *more,
):
    gx, gy, gz = lax.axis_index("gx"), lax.axis_index("gy"), lax.axis_index("gz")
    rows = cols.shape[3]
    size = tiles.shape[2]
    count = n_gx * rows
    chunks = window.shape[0]
    block = size // n_gy
    high = n_gy * SUB
    wide = rows // pieces
    broad = count // pieces
    steps = chunks * pieces
    f32, bf16 = jnp.float32, jnp.bfloat16

    first_load = pltpu.make_async_copy(tiles.at[pl.ds(0, slots)], held.at[pl.ds(0, slots)], load_sem.at[0])
    first_load.start()
    loads = [first_load]
    parts = load_sem.shape[0] - 1
    for part in range(parts):
        low, top = 1 + (rows - 1) * part // parts, 1 + (rows - 1) * (part + 1) // parts
        loads.append(pltpu.make_async_copy(
            tiles.at[pl.ds(low * slots, (top - low) * slots)], held.at[pl.ds(low * slots, (top - low) * slots)],
            load_sem.at[part + 1],
        ))
        loads[-1].start()
    enter = knock(("gx", "gy", "gz"), twos > 0)

    def win_copy(m, peer):
        return remote(window.at[m, gx], window.at[m, gx], win_send.at[peer], win_recv.at[m], "gy", peer)

    def fan_copy(m, d):
        return remote(window.at[m, gx], window.at[m, gx], fan_send.at[d - 1], fan_recv.at[m, d - 1],
                      "gx", lax.rem(gx + d, n_gx))

    def fan_landing(m, d):
        g = lax.rem(gx - d + n_gx, n_gx)
        return remote(window.at[m, g], window.at[m, g], fan_send.at[d - 1], fan_recv.at[m, d - 1],
                      "gx", lax.rem(gx + d, n_gx))

    def head_copy(peer):
        return remote(heads.at[gx], heads.at[gx], head_sem.at[0, peer], head_sem.at[1, 0], "gy", peer)

    def head_fan(d):
        return remote(heads.at[gx], heads.at[gx], head_side.at[0, d - 1], head_side.at[1, d - 1],
                      "gx", lax.rem(gx + d, n_gx))

    def head_landing(d):
        g = lax.rem(gx - d + n_gx, n_gx)
        return remote(heads.at[g], heads.at[g], head_side.at[0, d - 1], head_side.at[1, d - 1],
                      "gx", lax.rem(gx + d, n_gx))

    lanes = lax.broadcasted_iota(jnp.int32, (rows, LANES), 1)
    places = lax.broadcasted_iota(jnp.int32, (rows, LANES), 0)
    listed = cols[0, :, 0, :].T
    each = [jnp.broadcast_to(listed[:, k:k + 1], (rows, LANES)) for k in range(slots)]
    spread = jnp.full((rows, LANES), -1, jnp.int32)
    for k in range(slots):
        spread = jnp.where(lanes == k, each[k], spread)

    @pl.when(gy == 0)
    def _():
        heads[gx] = spread[:heads.shape[1]]
        first_load.wait()
        for k in range(slots):
            tile = held[k].astype(f32)
            for m in range(chunks):
                window[m, gx, k] = jnp.concatenate(
                    [tile[q * block + m * SUB:][:SUB] for q in range(n_gy)], axis=0
                ).astype(bf16)

    marks = [jnp.where(each[k] == lanes, places * SUB + k, -1) for k in range(slots)]
    lists_v[...] = jnp.zeros_like(lists_v)
    for i in range(slots):
        top = marks[0]
        for k in range(1, slots):
            top = jnp.maximum(top, marks[k])
        top = jnp.max(top, axis=0, keepdims=True)
        marks = [jnp.where(mark == top, -1, mark) for mark in marks]
        row, slot = top // SUB, top % SUB
        lists_v[i:i + 1] = jnp.where(top < 0, rows, row)
        lists_v[SUB + i:SUB + i + 1] = jnp.where(top < 0, 0, row * slots + slot)
    list_copy = pltpu.make_async_copy(lists_v, lists, table_sem.at[0])
    list_copy.start()
    enter()

    @pl.when(gy == 0)
    def _():
        for peer in range(1, n_gy):
            head_copy(peer).start()
        for d in range(1, n_gx):
            head_fan(d).start()
        for m in range(chunks):
            for peer in range(1, n_gy):
                win_copy(m, peer).start()
            for d in range(1, n_gx):
                fan_copy(m, d).start()

    for load in loads[1:]:
        load.wait()

    @pl.when(gy != 0)
    def _():
        first_load.wait()

    list_copy.wait()
    if twos:
        (seed, ids, lists2_v, lists2, listed_v, listed_s, product2, mixed2, side2_out, side2_in,
         last2_out, last2_in, gat, s2_out, s2_in, full, r_out, r_in, z_in,
         seed_send, seed_recv, ids_send, ids_recv, table2_sem, side2_send, side2_recv, last2_send, last2_recv,
         gat_send, gat_recv, s2_send, s2_recv, r_send, r_recv, z_send, z_recv) = more
        tall2 = twos * SUB
        high2 = n_gy * tall2
        down2 = pl.ds(block - tall2, tall2)
        plane = n_gy * n_gx
        me = gy * n_gx + gx
        seeds = seed_recv.shape[0]
        each_seed = slots // seeds
        per = pieces // r_recv.shape[0]
        listed_v[...] = spread
        listed_copy = pltpu.make_async_copy(listed_v, listed_s, table2_sem.at[0])
        listed_copy.start()
        seed[slots] = jnp.zeros((n_gx, high2, size), bf16)

        def seed_copy(p):
            part = seed.at[pl.ds(p * each_seed, each_seed)]
            return remote(part, part, seed_send, seed_recv.at[p], "gz", lax.rem(gz + 1, n_gz))

        def ids_copy(peer):
            return remote(lists_v.at[pl.ds(0, SUB)], ids, ids_send.at[peer], ids_recv, "gz", peer)

        @pl.when(gz == 0)
        def _():
            for peer in range(1, n_gz):
                ids_copy(peer).start()
            ids[...] = lists_v[0:SUB]
            across = lax.broadcasted_iota(jnp.int32, (high2, size), 1)
            at = lax.broadcasted_iota(jnp.int32, (high2, size), 0)
            pick = (at // tall2) * block + (block - tall2) + at % tall2
            pick = jnp.where(across == pick, 1.0, 0.0).astype(bf16)
            for p in range(seeds):
                for i in range(p * each_seed, (p + 1) * each_seed):
                    for g in range(n_gx):
                        tile = held[lists[SUB + i, g * rows]]
                        seed[i, g] = lax.dot_general(
                            pick, tile, (((1,), (1,)), ((), ())), preferred_element_type=f32
                        ).astype(bf16)
                seed_copy(p).start()

    for g in range(n_gx):
        for m in range(chunks):
            current[m, g, slots] = jnp.zeros((high, size), bf16)
    for parity in range(2):
        rounded[parity, rows] = jnp.zeros((n_gx * high, size), bf16)

    @pl.when(gy != 0)
    def _():
        head_copy(0).wait_recv()
        for d in range(1, n_gx):
            head_fan(d).start()

    for d in range(1, n_gx):
        head_landing(d).wait_recv()
    total = jnp.zeros((rows, LANES), jnp.int32)
    for g in range(n_gx):
        found = jnp.full((rows, LANES), slots, jnp.int32)
        for k in range(slots):
            found = jnp.where(spread == jnp.broadcast_to(heads[g, 0:1, k:k + 1], (rows, LANES)), k, found)
        found = jnp.where(lanes < slots, found, 0)
        total = total + (found if g == 0 else pltpu.roll(found, g * SUB, 1))
    table_v[...] = total
    table_copy = pltpu.make_async_copy(table_v, table, table_sem.at[1])
    table_copy.start()

    def forward(m):
        @pl.when(gy != 0)
        def _():
            win_copy(m, 0).wait_recv()
            for d in range(1, n_gx):
                fan_copy(m, d).start()

    forward(0)
    table_copy.wait()
    if twos:
        @pl.when(gz > 0)
        def _():
            ids_copy(0).wait_recv()

        mine = lists_v[0:SUB]
        for g in range(n_gx):
            found = jnp.full((SUB, LANES), slots, jnp.int32)
            for j in range(slots):
                label = jnp.broadcast_to(ids[j:j + 1, g * rows:g * rows + 1], (SUB, LANES))
                found = jnp.where(mine == label, j, found)
            lists2_v[g * SUB:(g + 1) * SUB] = jnp.where(mine >= rows, slots, found)
        lists2_copy = pltpu.make_async_copy(lists2_v, lists2, table2_sem.at[1])
        lists2_copy.start()
        listed_copy.wait()
        lists2_copy.wait()

    def right_copy(t):
        return remote(right_out.at[t], right_in.at[t], right_send, right_recv.at[t],
                      "gz", lax.rem(gz + 1, n_gz))

    def left_copy(t):
        return remote(left_out.at[t], left_in.at[t], left_send, left_recv.at[t],
                      "gz", lax.rem(gz + n_gz - 1, n_gz))

    def side_slot(u):
        return u if buffers == chunks else lax.rem(u, buffers * pieces)

    def side_sem(s):
        return 0 if buffers == chunks else s

    def side_all(u):
        s = side_slot(u)
        return remote(side_in.at[s], side_in.at[s], side_send.at[side_sem(s)], side_recv.at[s],
                      "gx", lax.rem(gx + 1, n_gx))

    def last_all(v):
        return remote(last_in.at[v], last_in.at[v], last_send, last_recv.at[v], "gy", lax.rem(gy + 1, n_gy))

    def side_copy(u, d):
        peer = lax.rem(gx + d, n_gx)
        s = side_slot(u)
        return remote(side_out.at[s, peer], side_in.at[s, d - 1], side_send.at[side_sem(s)], side_recv.at[s],
                      "gx", peer)

    def last_copy(v, d):
        peer = lax.rem(gy + d, n_gy)
        return remote(last_out.at[v, peer], last_in.at[v, d - 1], last_send, last_recv.at[v],
                      "gy", peer)

    def fetch(m):
        for d in range(1, n_gx):
            fan_landing(m, d).wait_recv()
        for g in range(n_gx):
            for k in range(slots):
                current[m, g, k] = window[m, g, k]

    def multiply(q, ms):
        for i in range(wide):
            c = q * wide + i
            lhs = jnp.concatenate([
                jnp.concatenate([current[m, g, table[c, g * SUB + j]] for m in ms for g in range(n_gx)], axis=0)
                for j in range(slots)
            ], axis=1)
            rhs = jnp.concatenate([held[c * slots + j] for j in range(slots)], axis=1)
            value = lax.dot_general(lhs, rhs, (((1,), (1,)), ((), ())), preferred_element_type=f32)
            for n, m in enumerate(ms):
                own[m * pieces + q, i] = value[n * n_gx * high:(n + 1) * n_gx * high]

    def stage_own(t):
        @pl.when((t > 0) & (t < chunks))
        def _():
            forward(t)

        spans = [[0], list(range(1, chunks))] if twos else [[m] for m in range(chunks)]
        for n, ms in enumerate(spans):
            @pl.when(t == n * pieces)
            def _():
                for m in ms:
                    fetch(m)

            @pl.when((t >= n * pieces) & (t < (n + 1) * pieces))
            def _():
                multiply(t - n * pieces, ms)

    def stage_right(t):
        @pl.when(gz == 0)
        def _():
            right_out[t] = own[t].astype(bf16)

        @pl.when(gz > 0)
        def _():
            right_copy(t).wait_recv()

        @pl.when((gz > 0) & (gz < n_gz - 1))
        def _():
            right_out[t] = (own[t] + right_in[t].astype(f32)).astype(bf16)

        @pl.when(gz < n_gz - 1)
        def _():
            right_copy(t).start()

    def stage_left(t):
        @pl.when(gz == n_gz - 1)
        def _():
            left_out[t] = own[t].astype(bf16)

        @pl.when(gz < n_gz - 1)
        def _():
            left_copy(t).wait_recv()

        @pl.when((gz > 0) & (gz < n_gz - 1))
        def _():
            left_out[t] = (own[t] + left_in[t].astype(f32)).astype(bf16)

        @pl.when(gz > 0)
        def _():
            left_copy(t).start()

    def stage_sum(t):
        parity, q = lax.rem(t // pieces, 2), lax.rem(t, pieces)

        def keep(total):
            square[parity, pl.ds(q * wide, wide)] = total
            rounded[parity, pl.ds(q * wide, wide)] = total.astype(bf16)

        @pl.when(gz == 0)
        def _():
            keep(own[t] + left_in[t].astype(f32))

        @pl.when(gz == n_gz - 1)
        def _():
            keep(own[t] + right_in[t].astype(f32))

        @pl.when((gz > 0) & (gz < n_gz - 1))
        def _():
            keep(own[t] + right_in[t].astype(f32) + left_in[t].astype(f32))

    def stage_second(u):
        parity, q = lax.rem(u // pieces, 2), lax.rem(u, pieces)
        depth = min(slots, rows)
        s = side_slot(u)
        hold = lax.rem(u, SIDE_LAG + 1)
        if buffers < chunks:
            @pl.when((q == 0) & (u >= buffers * pieces))
            def _():
                pl.semaphore_wait(credit, n_gx - 1)

            @pl.when(u >= buffers * pieces)
            def _():
                side_all(u).wait_send()

        for i in range(broad):
            c = q * broad + i
            lhs = jnp.concatenate([rounded[parity, lists[j, c]] for j in range(depth)], axis=1)
            rhs = jnp.concatenate([held[lists[SUB + j, c]] for j in range(depth)], axis=0)
            near = c - gx * rows
            here = (gy == gz) & (near >= 0) & (near < rows)
            near = jnp.clip(near, 0, rows - 1)
            value = (jnp.where(here, 3.0, 0.0) * square[parity, near]
                     - 2.0 * jnp.dot(lhs, rhs, preferred_element_type=f32))
            mine = value[:high]
            for g in range(1, n_gx):
                mine = jnp.where(gx == g, value[g * high:(g + 1) * high], mine)
            product[hold, i] = mine
            for g in range(n_gx):
                side_out[s, g, i] = value[g * high:(g + 1) * high].astype(bf16)
        for d in range(1, n_gx):
            side_copy(u, d).start()

    def stage_mix(v):
        m, q = v // pieces, lax.rem(v, pieces)
        hold = lax.rem(v, SIDE_LAG + 1)
        s = side_slot(v)
        side_all(v).wait_recv()
        for i in range(0, broad, 2):
            pair = []
            for h in range(i, i + 2):
                value = product[hold, h]
                for d in range(1, n_gx):
                    value = value + side_in[s, d - 1, h].astype(f32)
                mixed[h] = value
                pair.append(value)
            for y in range(n_gy):
                last_out[v // 2, y, lax.rem(v, 2), i // 2] = jnp.concatenate(
                    [value[y * SUB:(y + 1) * SUB] for value in pair], axis=0
                ).astype(bf16)

        @pl.when(lax.rem(v, 2) == 1)
        def _():
            for d in range(1, n_gy):
                last_copy(v // 2, d).start()

        if buffers < chunks:
            @pl.when((q == pieces - 1) & (m + buffers < chunks))
            def _():
                for d in range(1, n_gx):
                    pl.semaphore_signal(credit, inc=1, device_id={"gx": lax.rem(gx + d, n_gx)},
                                        device_id_type=MESH)
        down = pl.ds(pl.multiple_of(m * SUB, SUB), SUB)
        for i in range(broad):
            across = pl.ds(pl.multiple_of((q * broad + i) * size, size), size)
            out[down, across] = mixed[i, pl.ds(pl.multiple_of(gy * SUB, SUB), SUB)]

    def stage_last(w):
        m, q = w // pieces, lax.rem(w, pieces)
        down = pl.ds(pl.multiple_of(m * SUB, SUB), SUB)

        @pl.when(lax.rem(w, 2) == 1)
        def _():
            last_all(w // 2).wait_recv()
            for n in range(2):
                for i in range(0, broad, 2):
                    value = last_in[w // 2, 0, n, i // 2].astype(f32)
                    for d in range(2, n_gy):
                        value = value + last_in[w // 2, d - 1, n, i // 2].astype(f32)
                    for h in range(2):
                        across = pl.ds(pl.multiple_of(((q - 1 + n) * broad + i + h) * size, size), size)
                        out[down, across] += value[h * SUB:(h + 1) * SUB]

    def pass_seed(p):
        @pl.when(gz > 0)
        def _():
            seed_copy(p).wait_recv()

        @pl.when((gz > 0) & (gz < n_gz - 1))
        def _():
            seed_copy(p).start()

    def across_of(c):
        return pl.ds(pl.multiple_of(c * size, size), size)

    def side2_copy(q, d):
        peer = lax.rem(gx + d, n_gx)
        return remote(side2_out.at[q, peer], side2_in.at[q, d - 1], side2_send, side2_recv.at[q], "gx", peer)

    def last2_copy(q, d):
        peer = lax.rem(gy + d, n_gy)
        return remote(last2_out.at[q, peer], last2_in.at[q, d - 1], last2_send, last2_recv.at[q], "gy", peer)

    def gat_copy(q, d):
        return remote(gat.at[q, 0], gat.at[q, d], gat_send, gat_recv.at[q], "gy", lax.rem(gy + d, n_gy))

    def s2_copy(q, d):
        return remote(s2_out.at[q], s2_in.at[q, d - 1], s2_send, s2_recv.at[q], "gx", lax.rem(gx + d, n_gx))

    def wait_all(ref, send, recv):
        remote(ref, ref, send, recv, "gy", lax.rem(gy + 1, n_gy)).wait_recv()

    def turn_first(q):
        hold = lax.rem(q, SIDE_LAG + 1)
        depth = min(slots, rows)
        for i in range(broad):
            c = q * broad + i
            lhs = jnp.concatenate([
                jnp.concatenate([seed[lists2[g * SUB + j, c], g] for g in range(n_gx)], axis=0)
                for j in range(depth)
            ], axis=1)
            rhs = jnp.concatenate([held[lists[SUB + j, c]] for j in range(depth)], axis=0)
            value = jnp.dot(lhs, rhs, preferred_element_type=f32)
            mine = value[:high2]
            for g in range(1, n_gx):
                mine = jnp.where(gx == g, value[g * high2:(g + 1) * high2], mine)
            product2[hold, i] = mine
            for g in range(n_gx):
                side2_out[q, g, i] = value[g * high2:(g + 1) * high2].astype(bf16)
        for d in range(1, n_gx):
            side2_copy(q, d).start()

    def turn_mix(q):
        hold = lax.rem(q, SIDE_LAG + 1)
        wait_all(side2_in.at[q], side2_send, side2_recv.at[q])
        for i in range(broad):
            value = product2[hold, i]
            for d in range(1, n_gx):
                value = value + side2_in[q, d - 1, i].astype(f32)
            mixed2[i] = value
            for y in range(n_gy):
                last2_out[q, y, i] = value[y * tall2:(y + 1) * tall2].astype(bf16)
        for d in range(1, n_gy):
            last2_copy(q, d).start()
        for i in range(broad):
            out[down2, across_of(q * broad + i)] = mixed2[i, pl.ds(pl.multiple_of(gy * tall2, tall2), tall2)]

    def turn_last(q):
        wait_all(last2_in.at[q], last2_send, last2_recv.at[q])
        for i in range(broad):
            total = out[down2, across_of(q * broad + i)]
            for d in range(1, n_gy):
                total = total + last2_in[q, d - 1, i].astype(f32)
            gat[q, 0, i] = total.astype(bf16)
            out[down2, across_of(q * broad + i)] = 3.0 * total
        for d in range(1, n_gy):
            gat_copy(q, d).start()

    def turn_join(q):
        wait_all(gat.at[q, pl.ds(1, n_gy - 1)], gat_send, gat_recv.at[q])
        for i in range(broad):
            tile = jnp.concatenate([gat[q, lax.rem(gy - y + n_gy, n_gy), i] for y in range(n_gy)], axis=0)
            s2_out[q, i] = tile
            full[gx, q * broad + i] = tile
        for d in range(1, n_gx):
            s2_copy(q, d).start()

    def turn_collect(q):
        wait_all(s2_in.at[q], s2_send, s2_recv.at[q])
        for d in range(1, n_gx):
            g = lax.rem(gx - d + n_gx, n_gx)
            full[g, pl.ds(q * broad, broad)] = s2_in[q, d - 1]

    def turn_back(q):
        group = q // per
        for i in range(wide):
            c = q * wide + i
            lhs = jnp.concatenate([
                jnp.concatenate([full[g, listed_s[c, j]] for g in range(n_gx)], axis=0)
                for j in range(slots)
            ], axis=1)
            rhs = jnp.concatenate([held[c * slots + j] for j in range(slots)], axis=1)
            value = -2.0 * lax.dot_general(lhs, rhs, (((1,), (1,)), ((), ())), preferred_element_type=f32)
            for g in range(n_gx):
                for y in range(n_gy):
                    low = g * high2 + y * tall2
                    r_out[group, y * n_gx + g, lax.rem(q, per) * wide + i] = value[low:low + tall2].astype(bf16)

        @pl.when(lax.rem(q, per) == per - 1)
        def _():
            for d in range(1, plane):
                peer = lax.rem(me + d, plane)
                pltpu.make_async_remote_copy(
                    src_ref=r_out.at[group, peer], dst_ref=r_in.at[group, plane - d],
                    send_sem=r_send, recv_sem=r_recv.at[group],
                    device_id={"gx": lax.rem(peer, n_gx), "gy": peer // n_gx}, device_id_type=MESH,
                ).start()
            r_in[group, 0] = r_out[group, me]

    def from_slab(a, x):
        return lax.rem(a * n_gx + x - me + plane, plane)

    def turn_pass(q):
        group = q // per

        @pl.when(lax.rem(q, per) == per - 1)
        def _():
            wait_all(r_in.at[group, pl.ds(1, plane - 1)], r_send, r_recv.at[group])
            for d in range(1, n_gz):
                a = lax.rem(gz + d, n_gz)
                for x in range(n_gx):
                    remote(r_in.at[group, from_slab(a, x)], z_in.at[group, d - 1, x],
                           z_send, z_recv.at[group], "gz", a).start()

    def turn_end(q):
        group = q // per

        @pl.when(lax.rem(q, per) == 0)
        def _():
            wait_all(z_in.at[group], z_send, z_recv.at[group])

        for x in range(n_gx):
            for i in range(wide):
                n = lax.rem(q, per) * wide + i
                value = r_in[group, from_slab(gz, x), n].astype(f32)
                for d in range(1, n_gz):
                    value = value + z_in[group, d - 1, x, n].astype(f32)
                out[down2, across_of(x * rows + q * wide + i)] += value

    def hops(count, extra):
        return count * (HOP_LAG // 2) + (count + extra) // 2 * (HOP_LAG % 2)

    behind, ahead = gz, n_gz - 1 - gz
    right_at, left_at = hops(behind, 0), hops(ahead, n_gz % 2 + 1)
    sum_at = max(hops(n_gz - 1, 0), hops(n_gz - 1, n_gz % 2 + 1))
    second_at = sum_at + pieces - 1
    mix_at = second_at + SIDE_LAG
    last_at = mix_at + LAST_LAG

    stages = [
        (stage_own, 0, steps),
        (stage_right, right_at, steps),
        (stage_left, left_at, steps),
        (stage_sum, sum_at, steps),
        (stage_mix, mix_at, steps),
        (stage_second, second_at, steps),
        (stage_last, last_at, steps),
    ]
    slots_needed = steps + last_at
    if twos:
        turn_mix_at = TURN_AT + SIDE_LAG
        turn_last_at = turn_mix_at + TURN_LAST
        join_at = turn_last_at + JOIN_LAG
        collect_at = join_at + COLLECT_LAG
        back_at = collect_at + pieces - 1
        pass_at = back_at + PASS_LAG
        end_at = pass_at + END_LAG
        stages = stages[:4] + [
            (pass_seed, (gz - 1) * SEED_HOP, seeds),
            (stage_mix, mix_at, steps),
            (turn_mix, turn_mix_at, pieces),
            (turn_collect, collect_at, pieces),
            (turn_pass, pass_at, pieces),
            (turn_back, back_at, pieces),
            (stage_second, second_at, steps),
            (turn_first, TURN_AT, pieces),
            (stage_last, last_at, steps),
            (turn_last, turn_last_at, pieces),
            (turn_join, join_at, pieces),
            (turn_end, end_at, pieces),
        ]
        slots_needed = max(slots_needed, end_at + pieces)

    def slot(s, carry):
        for stage, delay, span in stages:
            t = s - delay
            pl.when((t >= 0) & (t < span))(functools.partial(stage, t))
        return carry

    lax.fori_loop(0, slots_needed, slot, jnp.int32(0))

    @pl.when(gz < n_gz - 1)
    def _():
        remote(right_out, right_out, right_send, right_recv.at[0], "gz", lax.rem(gz + 1, n_gz)).wait_send()

    @pl.when(gz > 0)
    def _():
        remote(left_out, left_out, left_send, left_recv.at[0], "gz", lax.rem(gz + n_gz - 1, n_gz)).wait_send()

    remote(last_in, last_in, last_send, last_recv.at[0], "gy", lax.rem(gy + 1, n_gy)).wait_send()
    if buffers == chunks:
        remote(side_in, side_in, side_send.at[0], side_recv.at[0], "gx", lax.rem(gx + 1, n_gx)).wait_send()
    else:
        @pl.loop(0, buffers * pieces)
        def _(t):
            side_all(t).wait_send()

    if twos:
        def sent(ref, send, recv):
            remote(ref, ref, send, recv, "gy", lax.rem(gy + 1, n_gy)).wait_send()

        sent(side2_in, side2_send, side2_recv.at[0])
        sent(last2_in, last2_send, last2_recv.at[0])
        sent(gat.at[:, pl.ds(1, n_gy - 1)], gat_send, gat_recv.at[0])
        sent(s2_in, s2_send, s2_recv.at[0])
        sent(r_in.at[:, pl.ds(1, plane - 1)], r_send, r_recv.at[0])
        sent(z_in, z_send, z_recv.at[0])

        @pl.when(gz < n_gz - 1)
        def _():
            sent(seed.at[pl.ds(0, slots)], seed_send, seed_recv.at[0])

        @pl.when(gz == 0)
        def _():
            for peer in range(1, n_gz):
                ids_copy(peer).wait_send()

    for d in range(1, n_gx):
        head_fan(d).wait_send()
        whole = window.at[:, gx]
        remote(whole, whole, fan_send.at[d - 1], fan_recv.at[0, d - 1], "gx", lax.rem(gx + d, n_gx)).wait_send()

    @pl.when(gy == 0)
    def _():
        for peer in range(1, n_gy):
            head_copy(peer).wait_send()
            whole = window.at[:, gx]
            remote(whole, whole, win_send.at[peer], win_recv.at[0], "gy", peer).wait_send()


def local(block_values, block_cols):
    n_gx, n_gy, n_gz = (lax.axis_size(a) for a in ("gx", "gy", "gz"))
    rows, slots = block_cols.shape[1], block_cols.shape[3]
    size = block_values.shape[4]
    tiles = block_values.reshape(rows * slots, size, size)
    count = n_gx * rows
    chunks = size // (n_gy * SUB)
    twos = 1 if n_gx <= 4 and chunks > 2 and n_gy == n_gz else 0
    chunks = chunks - twos
    high = n_gy * SUB
    pieces = pieces_of(rows, PIECES)
    wide, broad, steps = rows // pieces, count // pieces, chunks * pieces
    tall = n_gx * high
    buffers = chunks if n_gx <= 4 else 2
    top = min(SUB, rows)
    limit = VMEM if buffers < chunks else VMEM - 4 * rows * slots * size * size
    dma = pltpu.SemaphoreType.DMA
    f32, bf16 = jnp.float32, jnp.bfloat16
    flow = (steps, wide, tall, size)
    more = []
    if twos:
        tall2 = twos * SUB
        high2, plane, seeds = n_gy * tall2, n_gy * n_gx, pieces_of(slots, 3)
        groups = pieces_of(pieces, GROUPS)
        more = [
            pltpu.VMEM((slots + 1, n_gx, high2, size), bf16),
            pltpu.VMEM((SUB, LANES), jnp.int32),
            pltpu.VMEM((n_gx * SUB, LANES), jnp.int32),
            pltpu.SMEM((n_gx * SUB, LANES), jnp.int32),
            pltpu.VMEM((rows, LANES), jnp.int32),
            pltpu.SMEM((rows, LANES), jnp.int32),
            pltpu.VMEM((SIDE_LAG + 1, broad, high2, size), f32),
            pltpu.VMEM((broad, high2, size), f32),
            pltpu.VMEM((pieces, n_gx, broad, high2, size), bf16),
            pltpu.VMEM((pieces, n_gx - 1, broad, high2, size), bf16),
            pltpu.VMEM((pieces, n_gy, broad, tall2, size), bf16),
            pltpu.VMEM((pieces, n_gy - 1, broad, tall2, size), bf16),
            pltpu.VMEM((pieces, n_gy, broad, tall2, size), bf16),
            pltpu.VMEM((pieces, broad, high2, size), bf16),
            pltpu.VMEM((pieces, n_gx - 1, broad, high2, size), bf16),
            pltpu.VMEM((n_gx, count, high2, size), bf16),
            pltpu.VMEM((groups, plane, rows // groups, tall2, size), bf16),
            pltpu.VMEM((groups, plane, rows // groups, tall2, size), bf16),
            pltpu.VMEM((groups, n_gz - 1, n_gx, rows // groups, tall2, size), bf16),
            dma, dma((seeds,)), dma((n_gz,)), dma, dma((2,)),
            dma, dma((pieces,)), dma, dma((pieces,)), dma, dma((pieces,)),
            dma, dma((pieces,)), dma, dma((groups,)), dma, dma((groups,)),
        ]
    return pl.pallas_call(
        functools.partial(step_kernel, n_gx, n_gy, n_gz, slots, pieces, buffers, twos),
        out_shape=jax.ShapeDtypeStruct((size // n_gy, count * size), f32),
        in_specs=[pl.BlockSpec(memory_space=pl.ANY), pl.BlockSpec(memory_space=pltpu.VMEM)],
        out_specs=pl.BlockSpec(memory_space=pltpu.VMEM),
        scratch_shapes=[
            pltpu.VMEM((rows * slots, size, size), bf16),
            pltpu.VMEM((chunks, n_gx, slots, high, size), bf16),
            pltpu.VMEM((chunks, n_gx, slots + 1, high, size), bf16),
            pltpu.VMEM((n_gx, top, LANES), jnp.int32),
            pltpu.VMEM((rows, LANES), jnp.int32),
            pltpu.VMEM((2 * SUB, LANES), jnp.int32),
            pltpu.SMEM((rows, LANES), jnp.int32),
            pltpu.SMEM((2 * SUB, LANES), jnp.int32),
            pltpu.VMEM(flow, f32),
            pltpu.VMEM(flow, bf16), pltpu.VMEM(flow, bf16), pltpu.VMEM(flow, bf16), pltpu.VMEM(flow, bf16),
            pltpu.VMEM((2, rows, tall, size), f32),
            pltpu.VMEM((2, rows + 1, tall, size), bf16),
            pltpu.VMEM((SIDE_LAG + 1, broad, high, size), f32),
            pltpu.VMEM((buffers * pieces, n_gx, broad, high, size), bf16),
            pltpu.VMEM((buffers * pieces, n_gx - 1, broad, high, size), bf16),
            pltpu.VMEM((broad, high, size), f32),
            pltpu.VMEM((steps // 2, n_gy, 2, broad // 2, 2 * SUB, size), bf16),
            pltpu.VMEM((steps // 2, n_gy - 1, 2, broad // 2, 2 * SUB, size), bf16),
            dma((1 + min(4, rows - 1),)), dma((2, n_gy)), dma((2, n_gx - 1)),
            dma((n_gy,)), dma((chunks,)), dma((n_gx - 1,)), dma((chunks, n_gx - 1)), dma((2,)),
            dma, dma, dma((steps,)), dma((steps,)),
            dma((1 if buffers == chunks else buffers * pieces,)), dma((buffers * pieces,)),
            dma, dma((steps // 2,)),
            pltpu.SemaphoreType.REGULAR,
        ] + more,
        compiler_params=pltpu.CompilerParams(
            collective_id=0, has_side_effects=True, vmem_limit_bytes=limit
        ),
        name="purify",
    )(tiles, jnp.transpose(block_cols, (0, 3, 2, 1)))


def solution(mesh):
    in_specs = (P("gy", "gx", "gz", None, None, None), P("gy", "gx", "gz", None))
    out_specs = P(("gx", "gy"), "gz")
    return jax.shard_map(local, mesh=mesh, in_specs=in_specs, out_specs=out_specs, check_vma=False)
```

```python
import functools

import jax
import jax.numpy as jnp
from jax import lax
from jax.experimental import pallas as pl
from jax.experimental.pallas import tpu as pltpu
from jax.sharding import PartitionSpec as P

LANES = 128
SUB = 8
VMEM = 67043328
MESH = pl.DeviceIdType.MESH
HOP_LAG, SIDE_LAG, LAST_LAG = 6, 2, 6
SEED_HOP, TURN_AT, TURN_LAST, JOIN_LAG, COLLECT_LAG, PASS_LAG, END_LAG = 2, 6, 6, 4, 2, 5, 7
PIECES, GROUPS = 8, 4


def pieces_of(count, most):
    for pieces in range(min(count, most), 0, -1):
        if count % pieces == 0:
            return pieces


def knock(axes, plane):
    barrier = pltpu.get_barrier_semaphore()
    total = 0
    for axis in axes:
        size = lax.axis_size(axis)
        me = lax.axis_index(axis)
        for step in range(1, size):
            pl.semaphore_signal(
                barrier, inc=1, device_id={axis: lax.rem(me + step, size)}, device_id_type=MESH
            )
        total += size - 1
    if plane:
        n_gx, n_gy = lax.axis_size("gx"), lax.axis_size("gy")
        for dx in range(1, n_gx):
            for dy in range(1, n_gy):
                peer = {"gx": lax.rem(lax.axis_index("gx") + dx, n_gx),
                        "gy": lax.rem(lax.axis_index("gy") + dy, n_gy)}
                pl.semaphore_signal(barrier, inc=1, device_id=peer, device_id_type=MESH)
        total += (n_gx - 1) * (n_gy - 1)
    return lambda: pl.semaphore_wait(barrier, total)


def remote(src, dst, send, recv, axis, peer):
    return pltpu.make_async_remote_copy(
        src_ref=src, dst_ref=dst, send_sem=send, recv_sem=recv,
        device_id={axis: peer}, device_id_type=MESH,
    )


def step_kernel(
    n_gx, n_gy, n_gz, slots, pieces, buffers, twos,
    tiles, cols, out,
    held, window, current, heads, table_v, lists_v, table, lists,
    own, right_out, left_out, right_in, left_in, square, rounded,
    product, side_out, side_in, mixed, last_out, last_in,
    load_sem, head_sem, head_side, win_send, win_recv, fan_send, fan_recv, table_sem,
    right_send, left_send, right_recv, left_recv, side_send, side_recv, last_send, last_recv, credit,
    *more,
):
    gx, gy, gz = lax.axis_index("gx"), lax.axis_index("gy"), lax.axis_index("gz")
    rows = cols.shape[3]
    size = tiles.shape[2]
    count = n_gx * rows
    chunks = window.shape[0]
    block = size // n_gy
    high = n_gy * SUB
    wide = rows // pieces
    broad = count // pieces
    steps = chunks * pieces
    f32, bf16 = jnp.float32, jnp.bfloat16

    first_load = pltpu.make_async_copy(tiles.at[pl.ds(0, slots)], held.at[pl.ds(0, slots)], load_sem.at[0])
    first_load.start()
    loads = [first_load]
    parts = load_sem.shape[0] - 1
    for part in range(parts):
        low, top = 1 + (rows - 1) * part // parts, 1 + (rows - 1) * (part + 1) // parts
        loads.append(pltpu.make_async_copy(
            tiles.at[pl.ds(low * slots, (top - low) * slots)], held.at[pl.ds(low * slots, (top - low) * slots)],
            load_sem.at[part + 1],
        ))
        loads[-1].start()
    enter = knock(("gx", "gy", "gz"), twos > 0)

    def win_copy(m, peer):
        return remote(window.at[m, gx], window.at[m, gx], win_send.at[peer], win_recv.at[m], "gy", peer)

    def fan_copy(m, d):
        return remote(window.at[m, gx], window.at[m, gx], fan_send.at[d - 1], fan_recv.at[m, d - 1],
                      "gx", lax.rem(gx + d, n_gx))

    def fan_landing(m, d):
        g = lax.rem(gx - d + n_gx, n_gx)
        return remote(window.at[m, g], window.at[m, g], fan_send.at[d - 1], fan_recv.at[m, d - 1],
                      "gx", lax.rem(gx + d, n_gx))

    def head_copy(peer):
        return remote(heads.at[gx], heads.at[gx], head_sem.at[0, peer], head_sem.at[1, 0], "gy", peer)

    def head_fan(d):
        return remote(heads.at[gx], heads.at[gx], head_side.at[0, d - 1], head_side.at[1, d - 1],
                      "gx", lax.rem(gx + d, n_gx))

    def head_landing(d):
        g = lax.rem(gx - d + n_gx, n_gx)
        return remote(heads.at[g], heads.at[g], head_side.at[0, d - 1], head_side.at[1, d - 1],
                      "gx", lax.rem(gx + d, n_gx))

    lanes = lax.broadcasted_iota(jnp.int32, (rows, LANES), 1)
    places = lax.broadcasted_iota(jnp.int32, (rows, LANES), 0)
    listed = cols[0, :, 0, :].T
    each = [jnp.broadcast_to(listed[:, k:k + 1], (rows, LANES)) for k in range(slots)]
    spread = jnp.full((rows, LANES), -1, jnp.int32)
    for k in range(slots):
        spread = jnp.where(lanes == k, each[k], spread)

    @pl.when(gy == 0)
    def _():
        heads[gx] = spread[:heads.shape[1]]
        first_load.wait()
        for k in range(slots):
            tile = held[k].astype(f32)
            for m in range(chunks):
                window[m, gx, k] = jnp.concatenate(
                    [tile[q * block + m * SUB:][:SUB] for q in range(n_gy)], axis=0
                ).astype(bf16)

    marks = [jnp.where(each[k] == lanes, places * SUB + k, -1) for k in range(slots)]
    lists_v[...] = jnp.zeros_like(lists_v)
    for i in range(slots):
        top = marks[0]
        for k in range(1, slots):
            top = jnp.maximum(top, marks[k])
        top = jnp.max(top, axis=0, keepdims=True)
        marks = [jnp.where(mark == top, -1, mark) for mark in marks]
        row, slot = top // SUB, top % SUB
        lists_v[i:i + 1] = jnp.where(top < 0, rows, row)
        lists_v[SUB + i:SUB + i + 1] = jnp.where(top < 0, 0, row * slots + slot)
    list_copy = pltpu.make_async_copy(lists_v, lists, table_sem.at[0])
    list_copy.start()
    enter()

    @pl.when(gy == 0)
    def _():
        for peer in range(1, n_gy):
            head_copy(peer).start()
        for d in range(1, n_gx):
            head_fan(d).start()
        for m in range(chunks):
            for peer in range(1, n_gy):
                win_copy(m, peer).start()
            for d in range(1, n_gx):
                fan_copy(m, d).start()

    for load in loads[1:]:
        load.wait()

    @pl.when(gy != 0)
    def _():
        first_load.wait()

    list_copy.wait()
    if twos:
        (seed, ids, lists2_v, lists2, listed_v, listed_s, product2, mixed2, side2_out, side2_in,
         last2_out, last2_in, gat, s2_out, s2_in, full, r_out, r_in, z_in,
         seed_send, seed_recv, ids_send, ids_recv, table2_sem, side2_send, side2_recv, last2_send, last2_recv,
         gat_send, gat_recv, s2_send, s2_recv, r_send, r_recv, z_send, z_recv) = more
        tall2 = twos * SUB
        high2 = n_gy * tall2
        down2 = pl.ds(block - tall2, tall2)
        plane = n_gy * n_gx
        me = gy * n_gx + gx
        seeds = seed_recv.shape[0]
        each_seed = slots // seeds
        per = pieces // r_recv.shape[0]
        listed_v[...] = spread
        listed_copy = pltpu.make_async_copy(listed_v, listed_s, table2_sem.at[0])
        listed_copy.start()
        seed[slots] = jnp.zeros((n_gx, high2, size), bf16)

        def seed_copy(p):
            part = seed.at[pl.ds(p * each_seed, each_seed)]
            return remote(part, part, seed_send, seed_recv.at[p], "gz", lax.rem(gz + 1, n_gz))

        def ids_copy(peer):
            return remote(lists_v.at[pl.ds(0, SUB)], ids, ids_send.at[peer], ids_recv, "gz", peer)

        @pl.when(gz == 0)
        def _():
            for peer in range(1, n_gz):
                ids_copy(peer).start()
            ids[...] = lists_v[0:SUB]
            across = lax.broadcasted_iota(jnp.int32, (high2, size), 1)
            at = lax.broadcasted_iota(jnp.int32, (high2, size), 0)
            pick = (at // tall2) * block + (block - tall2) + at % tall2
            pick = jnp.where(across == pick, 1.0, 0.0).astype(bf16)
            for p in range(seeds):
                for i in range(p * each_seed, (p + 1) * each_seed):
                    for g in range(n_gx):
                        tile = held[lists[SUB + i, g * rows]]
                        seed[i, g] = lax.dot_general(
                            pick, tile, (((1,), (1,)), ((), ())), preferred_element_type=f32
                        ).astype(bf16)
                seed_copy(p).start()

    for g in range(n_gx):
        for m in range(chunks):
            current[m, g, slots] = jnp.zeros((high, size), bf16)
    for parity in range(2):
        rounded[parity, rows] = jnp.zeros((n_gx * high, size), bf16)

    @pl.when(gy != 0)
    def _():
        head_copy(0).wait_recv()
        for d in range(1, n_gx):
            head_fan(d).start()

    for d in range(1, n_gx):
        head_landing(d).wait_recv()
    total = jnp.zeros((rows, LANES), jnp.int32)
    for g in range(n_gx):
        found = jnp.full((rows, LANES), slots, jnp.int32)
        for k in range(slots):
            found = jnp.where(spread == jnp.broadcast_to(heads[g, 0:1, k:k + 1], (rows, LANES)), k, found)
        found = jnp.where(lanes < slots, found, 0)
        total = total + (found if g == 0 else pltpu.roll(found, g * SUB, 1))
    table_v[...] = total
    table_copy = pltpu.make_async_copy(table_v, table, table_sem.at[1])
    table_copy.start()

    def forward(m):
        @pl.when(gy != 0)
        def _():
            win_copy(m, 0).wait_recv()
            for d in range(1, n_gx):
                fan_copy(m, d).start()

    forward(0)
    table_copy.wait()
    if twos:
        @pl.when(gz > 0)
        def _():
            ids_copy(0).wait_recv()

        mine = lists_v[0:SUB]
        for g in range(n_gx):
            found = jnp.full((SUB, LANES), slots, jnp.int32)
            for j in range(slots):
                label = jnp.broadcast_to(ids[j:j + 1, g * rows:g * rows + 1], (SUB, LANES))
                found = jnp.where(mine == label, j, found)
            lists2_v[g * SUB:(g + 1) * SUB] = jnp.where(mine >= rows, slots, found)
        lists2_copy = pltpu.make_async_copy(lists2_v, lists2, table2_sem.at[1])
        lists2_copy.start()
        listed_copy.wait()
        lists2_copy.wait()

    def right_copy(t):
        return remote(right_out.at[t], right_in.at[t], right_send, right_recv.at[t],
                      "gz", lax.rem(gz + 1, n_gz))

    def left_copy(t):
        return remote(left_out.at[t], left_in.at[t], left_send, left_recv.at[t],
                      "gz", lax.rem(gz + n_gz - 1, n_gz))

    def side_slot(u):
        return u if buffers == chunks else lax.rem(u, buffers * pieces)

    def side_sem(s):
        return 0 if buffers == chunks else s

    def side_all(u):
        s = side_slot(u)
        return remote(side_in.at[s], side_in.at[s], side_send.at[side_sem(s)], side_recv.at[s],
                      "gx", lax.rem(gx + 1, n_gx))

    def last_all(v):
        return remote(last_in.at[v], last_in.at[v], last_send, last_recv.at[v], "gy", lax.rem(gy + 1, n_gy))

    def side_copy(u, d):
        peer = lax.rem(gx + d, n_gx)
        s = side_slot(u)
        return remote(side_out.at[s, peer], side_in.at[s, d - 1], side_send.at[side_sem(s)], side_recv.at[s],
                      "gx", peer)

    def last_copy(v, d):
        peer = lax.rem(gy + d, n_gy)
        return remote(last_out.at[v, peer], last_in.at[v, d - 1], last_send, last_recv.at[v],
                      "gy", peer)

    def fetch(m):
        for d in range(1, n_gx):
            fan_landing(m, d).wait_recv()
        for g in range(n_gx):
            for k in range(slots):
                current[m, g, k] = window[m, g, k]

    def multiply(q, ms):
        for i in range(wide):
            c = q * wide + i
            lhs = jnp.concatenate([
                jnp.concatenate([current[m, g, table[c, g * SUB + j]] for m in ms for g in range(n_gx)], axis=0)
                for j in range(slots)
            ], axis=1)
            rhs = jnp.concatenate([held[c * slots + j] for j in range(slots)], axis=1)
            value = lax.dot_general(lhs, rhs, (((1,), (1,)), ((), ())), preferred_element_type=f32)
            for n, m in enumerate(ms):
                own[m * pieces + q, i] = value[n * n_gx * high:(n + 1) * n_gx * high]

    def stage_own(t):
        @pl.when((t > 0) & (t < chunks))
        def _():
            forward(t)

        spans = [[0], list(range(1, chunks))] if twos else [[m] for m in range(chunks)]
        for n, ms in enumerate(spans):
            @pl.when(t == n * pieces)
            def _():
                for m in ms:
                    fetch(m)

            @pl.when((t >= n * pieces) & (t < (n + 1) * pieces))
            def _():
                multiply(t - n * pieces, ms)

    def stage_right(t):
        @pl.when(gz == 0)
        def _():
            right_out[t] = own[t].astype(bf16)

        @pl.when(gz > 0)
        def _():
            right_copy(t).wait_recv()

        @pl.when((gz > 0) & (gz < n_gz - 1))
        def _():
            right_out[t] = (own[t] + right_in[t].astype(f32)).astype(bf16)

        @pl.when(gz < n_gz - 1)
        def _():
            right_copy(t).start()

    def stage_left(t):
        @pl.when(gz == n_gz - 1)
        def _():
            left_out[t] = own[t].astype(bf16)

        @pl.when(gz < n_gz - 1)
        def _():
            left_copy(t).wait_recv()

        @pl.when((gz > 0) & (gz < n_gz - 1))
        def _():
            left_out[t] = (own[t] + left_in[t].astype(f32)).astype(bf16)

        @pl.when(gz > 0)
        def _():
            left_copy(t).start()

    def stage_sum(t):
        parity, q = lax.rem(t // pieces, 2), lax.rem(t, pieces)

        def keep(total):
            square[parity, pl.ds(q * wide, wide)] = total
            rounded[parity, pl.ds(q * wide, wide)] = total.astype(bf16)

        @pl.when(gz == 0)
        def _():
            keep(own[t] + left_in[t].astype(f32))

        @pl.when(gz == n_gz - 1)
        def _():
            keep(own[t] + right_in[t].astype(f32))

        @pl.when((gz > 0) & (gz < n_gz - 1))
        def _():
            keep(own[t] + right_in[t].astype(f32) + left_in[t].astype(f32))

    def stage_second(u):
        parity, q = lax.rem(u // pieces, 2), lax.rem(u, pieces)
        depth = min(slots, rows)
        s = side_slot(u)
        hold = lax.rem(u, SIDE_LAG + 1)
        if buffers < chunks:
            @pl.when((q == 0) & (u >= buffers * pieces))
            def _():
                pl.semaphore_wait(credit, n_gx - 1)

            @pl.when(u >= buffers * pieces)
            def _():
                side_all(u).wait_send()

        for i in range(broad):
            c = q * broad + i
            lhs = jnp.concatenate([rounded[parity, lists[j, c]] for j in range(depth)], axis=1)
            rhs = jnp.concatenate([held[lists[SUB + j, c]] for j in range(depth)], axis=0)
            near = c - gx * rows
            here = (gy == gz) & (near >= 0) & (near < rows)
            near = jnp.clip(near, 0, rows - 1)
            value = (jnp.where(here, 3.0, 0.0) * square[parity, near]
                     - 2.0 * jnp.dot(lhs, rhs, preferred_element_type=f32))
            mine = value[:high]
            for g in range(1, n_gx):
                mine = jnp.where(gx == g, value[g * high:(g + 1) * high], mine)
            product[hold, i] = mine
            for g in range(n_gx):
                side_out[s, g, i] = value[g * high:(g + 1) * high].astype(bf16)
        for d in range(1, n_gx):
            side_copy(u, d).start()

    def stage_mix(v):
        m, q = v // pieces, lax.rem(v, pieces)
        hold = lax.rem(v, SIDE_LAG + 1)
        s = side_slot(v)
        side_all(v).wait_recv()
        for i in range(0, broad, 2):
            pair = []
            for h in range(i, i + 2):
                value = product[hold, h]
                for d in range(1, n_gx):
                    value = value + side_in[s, d - 1, h].astype(f32)
                mixed[h] = value
                pair.append(value)
            for y in range(n_gy):
                last_out[v // 2, y, lax.rem(v, 2), i // 2] = jnp.concatenate(
                    [value[y * SUB:(y + 1) * SUB] for value in pair], axis=0
                ).astype(bf16)

        @pl.when(lax.rem(v, 2) == 1)
        def _():
            for d in range(1, n_gy):
                last_copy(v // 2, d).start()

        if buffers < chunks:
            @pl.when((q == pieces - 1) & (m + buffers < chunks))
            def _():
                for d in range(1, n_gx):
                    pl.semaphore_signal(credit, inc=1, device_id={"gx": lax.rem(gx + d, n_gx)},
                                        device_id_type=MESH)
        down = pl.ds(pl.multiple_of(m * SUB, SUB), SUB)
        for i in range(broad):
            across = pl.ds(pl.multiple_of((q * broad + i) * size, size), size)
            out[down, across] = mixed[i, pl.ds(pl.multiple_of(gy * SUB, SUB), SUB)]

    def stage_last(w):
        m, q = w // pieces, lax.rem(w, pieces)
        down = pl.ds(pl.multiple_of(m * SUB, SUB), SUB)

        @pl.when(lax.rem(w, 2) == 1)
        def _():
            last_all(w // 2).wait_recv()
            for n in range(2):
                for i in range(0, broad, 2):
                    value = last_in[w // 2, 0, n, i // 2].astype(f32)
                    for d in range(2, n_gy):
                        value = value + last_in[w // 2, d - 1, n, i // 2].astype(f32)
                    for h in range(2):
                        across = pl.ds(pl.multiple_of(((q - 1 + n) * broad + i + h) * size, size), size)
                        out[down, across] += value[h * SUB:(h + 1) * SUB]

    def pass_seed(p):
        @pl.when(gz > 0)
        def _():
            seed_copy(p).wait_recv()

        @pl.when((gz > 0) & (gz < n_gz - 1))
        def _():
            seed_copy(p).start()

    def across_of(c):
        return pl.ds(pl.multiple_of(c * size, size), size)

    def side2_copy(q, d):
        peer = lax.rem(gx + d, n_gx)
        return remote(side2_out.at[q, peer], side2_in.at[q, d - 1], side2_send, side2_recv.at[q], "gx", peer)

    def last2_copy(q, d):
        peer = lax.rem(gy + d, n_gy)
        return remote(last2_out.at[q, peer], last2_in.at[q, d - 1], last2_send, last2_recv.at[q], "gy", peer)

    def gat_copy(q, d):
        return remote(gat.at[q, 0], gat.at[q, d], gat_send, gat_recv.at[q], "gy", lax.rem(gy + d, n_gy))

    def s2_copy(q, d):
        return remote(s2_out.at[q], s2_in.at[q, d - 1], s2_send, s2_recv.at[q], "gx", lax.rem(gx + d, n_gx))

    def wait_all(ref, send, recv):
        remote(ref, ref, send, recv, "gy", lax.rem(gy + 1, n_gy)).wait_recv()

    def turn_first(q):
        hold = lax.rem(q, SIDE_LAG + 1)
        depth = min(slots, rows)
        for i in range(broad):
            c = q * broad + i
            lhs = jnp.concatenate([
                jnp.concatenate([seed[lists2[g * SUB + j, c], g] for g in range(n_gx)], axis=0)
                for j in range(depth)
            ], axis=1)
            rhs = jnp.concatenate([held[lists[SUB + j, c]] for j in range(depth)], axis=0)
            value = jnp.dot(lhs, rhs, preferred_element_type=f32)
            mine = value[:high2]
            for g in range(1, n_gx):
                mine = jnp.where(gx == g, value[g * high2:(g + 1) * high2], mine)
            product2[hold, i] = mine
            for g in range(n_gx):
                side2_out[q, g, i] = value[g * high2:(g + 1) * high2].astype(bf16)
        for d in range(1, n_gx):
            side2_copy(q, d).start()

    def turn_mix(q):
        hold = lax.rem(q, SIDE_LAG + 1)
        wait_all(side2_in.at[q], side2_send, side2_recv.at[q])
        for i in range(broad):
            value = product2[hold, i]
            for d in range(1, n_gx):
                value = value + side2_in[q, d - 1, i].astype(f32)
            mixed2[i] = value
            for y in range(n_gy):
                last2_out[q, y, i] = value[y * tall2:(y + 1) * tall2].astype(bf16)
        for d in range(1, n_gy):
            last2_copy(q, d).start()
        for i in range(broad):
            out[down2, across_of(q * broad + i)] = mixed2[i, pl.ds(pl.multiple_of(gy * tall2, tall2), tall2)]

    def turn_last(q):
        wait_all(last2_in.at[q], last2_send, last2_recv.at[q])
        for i in range(broad):
            total = out[down2, across_of(q * broad + i)]
            for d in range(1, n_gy):
                total = total + last2_in[q, d - 1, i].astype(f32)
            gat[q, 0, i] = total.astype(bf16)
            out[down2, across_of(q * broad + i)] = 3.0 * total
        for d in range(1, n_gy):
            gat_copy(q, d).start()

    def turn_join(q):
        wait_all(gat.at[q, pl.ds(1, n_gy - 1)], gat_send, gat_recv.at[q])
        for i in range(broad):
            tile = jnp.concatenate([gat[q, lax.rem(gy - y + n_gy, n_gy), i] for y in range(n_gy)], axis=0)
            s2_out[q, i] = tile
            full[gx, q * broad + i] = tile
        for d in range(1, n_gx):
            s2_copy(q, d).start()

    def turn_collect(q):
        wait_all(s2_in.at[q], s2_send, s2_recv.at[q])
        for d in range(1, n_gx):
            g = lax.rem(gx - d + n_gx, n_gx)
            full[g, pl.ds(q * broad, broad)] = s2_in[q, d - 1]

    def turn_back(q):
        group = q // per
        for i in range(wide):
            c = q * wide + i
            lhs = jnp.concatenate([
                jnp.concatenate([full[g, listed_s[c, j]] for g in range(n_gx)], axis=0)
                for j in range(slots)
            ], axis=1)
            rhs = jnp.concatenate([held[c * slots + j] for j in range(slots)], axis=1)
            value = -2.0 * lax.dot_general(lhs, rhs, (((1,), (1,)), ((), ())), preferred_element_type=f32)
            for g in range(n_gx):
                for y in range(n_gy):
                    low = g * high2 + y * tall2
                    r_out[group, y * n_gx + g, lax.rem(q, per) * wide + i] = value[low:low + tall2].astype(bf16)

        @pl.when(lax.rem(q, per) == per - 1)
        def _():
            for d in range(1, plane):
                peer = lax.rem(me + d, plane)
                pltpu.make_async_remote_copy(
                    src_ref=r_out.at[group, peer], dst_ref=r_in.at[group, plane - d],
                    send_sem=r_send, recv_sem=r_recv.at[group],
                    device_id={"gx": lax.rem(peer, n_gx), "gy": peer // n_gx}, device_id_type=MESH,
                ).start()
            r_in[group, 0] = r_out[group, me]

    def from_slab(a, x):
        return lax.rem(a * n_gx + x - me + plane, plane)

    def turn_pass(q):
        group = q // per

        @pl.when(lax.rem(q, per) == per - 1)
        def _():
            wait_all(r_in.at[group, pl.ds(1, plane - 1)], r_send, r_recv.at[group])
            for d in range(1, n_gz):
                a = lax.rem(gz + d, n_gz)
                for x in range(n_gx):
                    remote(r_in.at[group, from_slab(a, x)], z_in.at[group, d - 1, x],
                           z_send, z_recv.at[group], "gz", a).start()

    def turn_end(q):
        group = q // per

        @pl.when(lax.rem(q, per) == 0)
        def _():
            wait_all(z_in.at[group], z_send, z_recv.at[group])

        for x in range(n_gx):
            for i in range(wide):
                n = lax.rem(q, per) * wide + i
                value = r_in[group, from_slab(gz, x), n].astype(f32)
                for d in range(1, n_gz):
                    value = value + z_in[group, d - 1, x, n].astype(f32)
                out[down2, across_of(x * rows + q * wide + i)] += value

    def hops(count, extra):
        return count * (HOP_LAG // 2) + (count + extra) // 2 * (HOP_LAG % 2)

    behind, ahead = gz, n_gz - 1 - gz
    right_at, left_at = hops(behind, 0), hops(ahead, n_gz % 2 + 1)
    farthest = max(hops(n_gz - 1, 0), hops(n_gz - 1, n_gz % 2 + 1))
    sum_at = jnp.maximum(right_at, left_at)
    second_at = sum_at + pieces - 1
    mix_at = second_at + SIDE_LAG
    last_at = mix_at + LAST_LAG

    stages = [
        (stage_own, 0, steps),
        (stage_right, right_at, steps),
        (stage_left, left_at, steps),
        (stage_sum, sum_at, steps),
        (stage_mix, mix_at, steps),
        (stage_second, second_at, steps),
        (stage_last, last_at, steps),
    ]
    slots_needed = steps + farthest + pieces - 1 + SIDE_LAG + LAST_LAG
    if twos:
        turn_mix_at = TURN_AT + SIDE_LAG
        turn_last_at = turn_mix_at + TURN_LAST
        join_at = turn_last_at + JOIN_LAG
        collect_at = join_at + COLLECT_LAG
        back_at = collect_at + pieces - 1
        pass_at = back_at + PASS_LAG
        end_at = pass_at + END_LAG
        stages = stages[:4] + [
            (pass_seed, (gz - 1) * SEED_HOP, seeds),
            (stage_mix, mix_at, steps),
            (turn_mix, turn_mix_at, pieces),
            (turn_collect, collect_at, pieces),
            (turn_pass, pass_at, pieces),
            (turn_back, back_at, pieces),
            (stage_second, second_at, steps),
            (turn_first, TURN_AT, pieces),
            (stage_last, last_at, steps),
            (turn_last, turn_last_at, pieces),
            (turn_join, join_at, pieces),
            (turn_end, end_at, pieces),
        ]
        slots_needed = max(slots_needed, end_at + pieces)

    def slot(s, carry):
        for stage, delay, span in stages:
            t = s - delay
            pl.when((t >= 0) & (t < span))(functools.partial(stage, t))
        return carry

    lax.fori_loop(0, slots_needed, slot, jnp.int32(0))

    @pl.when(gz < n_gz - 1)
    def _():
        remote(right_out, right_out, right_send, right_recv.at[0], "gz", lax.rem(gz + 1, n_gz)).wait_send()

    @pl.when(gz > 0)
    def _():
        remote(left_out, left_out, left_send, left_recv.at[0], "gz", lax.rem(gz + n_gz - 1, n_gz)).wait_send()

    remote(last_in, last_in, last_send, last_recv.at[0], "gy", lax.rem(gy + 1, n_gy)).wait_send()
    if buffers == chunks:
        remote(side_in, side_in, side_send.at[0], side_recv.at[0], "gx", lax.rem(gx + 1, n_gx)).wait_send()
    else:
        @pl.loop(0, buffers * pieces)
        def _(t):
            side_all(t).wait_send()

    if twos:
        def sent(ref, send, recv):
            remote(ref, ref, send, recv, "gy", lax.rem(gy + 1, n_gy)).wait_send()

        sent(side2_in, side2_send, side2_recv.at[0])
        sent(last2_in, last2_send, last2_recv.at[0])
        sent(gat.at[:, pl.ds(1, n_gy - 1)], gat_send, gat_recv.at[0])
        sent(s2_in, s2_send, s2_recv.at[0])
        sent(r_in.at[:, pl.ds(1, plane - 1)], r_send, r_recv.at[0])
        sent(z_in, z_send, z_recv.at[0])

        @pl.when(gz < n_gz - 1)
        def _():
            sent(seed.at[pl.ds(0, slots)], seed_send, seed_recv.at[0])

        @pl.when(gz == 0)
        def _():
            for peer in range(1, n_gz):
                ids_copy(peer).wait_send()

    for d in range(1, n_gx):
        head_fan(d).wait_send()
        whole = window.at[:, gx]
        remote(whole, whole, fan_send.at[d - 1], fan_recv.at[0, d - 1], "gx", lax.rem(gx + d, n_gx)).wait_send()

    @pl.when(gy == 0)
    def _():
        for peer in range(1, n_gy):
            head_copy(peer).wait_send()
            whole = window.at[:, gx]
            remote(whole, whole, win_send.at[peer], win_recv.at[0], "gy", peer).wait_send()


def local(block_values, block_cols):
    n_gx, n_gy, n_gz = (lax.axis_size(a) for a in ("gx", "gy", "gz"))
    rows, slots = block_cols.shape[1], block_cols.shape[3]
    size = block_values.shape[4]
    tiles = block_values.reshape(rows * slots, size, size)
    count = n_gx * rows
    chunks = size // (n_gy * SUB)
    twos = 1 if n_gx <= 4 and chunks > 2 and n_gy == n_gz else 0
    chunks = chunks - twos
    high = n_gy * SUB
    pieces = pieces_of(rows, PIECES)
    wide, broad, steps = rows // pieces, count // pieces, chunks * pieces
    tall = n_gx * high
    buffers = chunks if n_gx <= 4 else 2
    top = min(SUB, rows)
    limit = VMEM if buffers < chunks else VMEM - 4 * rows * slots * size * size
    dma = pltpu.SemaphoreType.DMA
    f32, bf16 = jnp.float32, jnp.bfloat16
    flow = (steps, wide, tall, size)
    more = []
    if twos:
        tall2 = twos * SUB
        high2, plane, seeds = n_gy * tall2, n_gy * n_gx, pieces_of(slots, 3)
        groups = pieces_of(pieces, GROUPS)
        more = [
            pltpu.VMEM((slots + 1, n_gx, high2, size), bf16),
            pltpu.VMEM((SUB, LANES), jnp.int32),
            pltpu.VMEM((n_gx * SUB, LANES), jnp.int32),
            pltpu.SMEM((n_gx * SUB, LANES), jnp.int32),
            pltpu.VMEM((rows, LANES), jnp.int32),
            pltpu.SMEM((rows, LANES), jnp.int32),
            pltpu.VMEM((SIDE_LAG + 1, broad, high2, size), f32),
            pltpu.VMEM((broad, high2, size), f32),
            pltpu.VMEM((pieces, n_gx, broad, high2, size), bf16),
            pltpu.VMEM((pieces, n_gx - 1, broad, high2, size), bf16),
            pltpu.VMEM((pieces, n_gy, broad, tall2, size), bf16),
            pltpu.VMEM((pieces, n_gy - 1, broad, tall2, size), bf16),
            pltpu.VMEM((pieces, n_gy, broad, tall2, size), bf16),
            pltpu.VMEM((pieces, broad, high2, size), bf16),
            pltpu.VMEM((pieces, n_gx - 1, broad, high2, size), bf16),
            pltpu.VMEM((n_gx, count, high2, size), bf16),
            pltpu.VMEM((groups, plane, rows // groups, tall2, size), bf16),
            pltpu.VMEM((groups, plane, rows // groups, tall2, size), bf16),
            pltpu.VMEM((groups, n_gz - 1, n_gx, rows // groups, tall2, size), bf16),
            dma, dma((seeds,)), dma((n_gz,)), dma, dma((2,)),
            dma, dma((pieces,)), dma, dma((pieces,)), dma, dma((pieces,)),
            dma, dma((pieces,)), dma, dma((groups,)), dma, dma((groups,)),
        ]
    return pl.pallas_call(
        functools.partial(step_kernel, n_gx, n_gy, n_gz, slots, pieces, buffers, twos),
        out_shape=jax.ShapeDtypeStruct((size // n_gy, count * size), f32),
        in_specs=[pl.BlockSpec(memory_space=pl.ANY), pl.BlockSpec(memory_space=pltpu.VMEM)],
        out_specs=pl.BlockSpec(memory_space=pltpu.VMEM),
        scratch_shapes=[
            pltpu.VMEM((rows * slots, size, size), bf16),
            pltpu.VMEM((chunks, n_gx, slots, high, size), bf16),
            pltpu.VMEM((chunks, n_gx, slots + 1, high, size), bf16),
            pltpu.VMEM((n_gx, top, LANES), jnp.int32),
            pltpu.VMEM((rows, LANES), jnp.int32),
            pltpu.VMEM((2 * SUB, LANES), jnp.int32),
            pltpu.SMEM((rows, LANES), jnp.int32),
            pltpu.SMEM((2 * SUB, LANES), jnp.int32),
            pltpu.VMEM(flow, f32),
            pltpu.VMEM(flow, bf16), pltpu.VMEM(flow, bf16), pltpu.VMEM(flow, bf16), pltpu.VMEM(flow, bf16),
            pltpu.VMEM((2, rows, tall, size), f32),
            pltpu.VMEM((2, rows + 1, tall, size), bf16),
            pltpu.VMEM((SIDE_LAG + 1, broad, high, size), f32),
            pltpu.VMEM((buffers * pieces, n_gx, broad, high, size), bf16),
            pltpu.VMEM((buffers * pieces, n_gx - 1, broad, high, size), bf16),
            pltpu.VMEM((broad, high, size), f32),
            pltpu.VMEM((steps // 2, n_gy, 2, broad // 2, 2 * SUB, size), bf16),
            pltpu.VMEM((steps // 2, n_gy - 1, 2, broad // 2, 2 * SUB, size), bf16),
            dma((1 + min(4, rows - 1),)), dma((2, n_gy)), dma((2, n_gx - 1)),
            dma((n_gy,)), dma((chunks,)), dma((n_gx - 1,)), dma((chunks, n_gx - 1)), dma((2,)),
            dma, dma, dma((steps,)), dma((steps,)),
            dma((1 if buffers == chunks else buffers * pieces,)), dma((buffers * pieces,)),
            dma, dma((steps // 2,)),
            pltpu.SemaphoreType.REGULAR,
        ] + more,
        compiler_params=pltpu.CompilerParams(
            collective_id=0, has_side_effects=True, vmem_limit_bytes=limit
        ),
        name="purify",
    )(tiles, jnp.transpose(block_cols, (0, 3, 2, 1)))


def solution(mesh):
    in_specs = (P("gy", "gx", "gz", None, None, None), P("gy", "gx", "gz", None))
    out_specs = P(("gx", "gy"), "gz")
    return jax.shard_map(local, mesh=mesh, in_specs=in_specs, out_specs=out_specs, check_vma=False)
```
